512 devices in a mesh: group: 16 (over z, core), panel: 32 (over x, y).
Axes of the slice: x: 4, y: 8, z: 8, core: 2. Of those that a mesh axis runs over, the one named last changes fastest.
Arguments:
- source_matrix_tiles: bfloat16 [2, 192, 4, 4096], P(None, 'group', None, 'panel'), may hold values from -6 to 6
- second_operand_encoded: bfloat16 [32, 4096, 2, 4096], P('group', None, None, 'panel'), may hold values from -0.5 to 0.5
- responding_nodes: int32 [19], replicated, may hold values from 0 to 31, as said below
Outputs:
- c_blocks: float32 [2, 192, 2, 4096], P(None, 'group', None, 'panel')
The draws below stay inside these ranges and needn't reach their ends.
Inputs may be any that keep to these rules, and one draw needn't show every extreme that they name: `responding_nodes`: 19 distinct point indices in ascending order; of the points 2 j and 2 j + 1, at least one is listed.
All inputs are finite; a program needn't handle non-finite values.
Results may differ from the reference program's by a relative error of at most 0.0029.
Values may be sent and summed in bfloat16 or wider, within the bound.
No kernel may reach another device: no remote copies, remote signals or barrier semaphores. Data moves between devices by JAX's collectives and lax.ppermute only.
A program may use at most 64 MiB of HBM per device.

```python
import math
import jax
import jax.numpy as jnp
from jax import lax

INNER = 16384
COLS = 8192
NODE_NUMBER = 32
SURV = 19
ROWS_HALF = 192


def remaining_points(key):
    pair_count = NODE_NUMBER // 2
    lagging_pairs = NODE_NUMBER - SURV
    ranking = jax.random.permutation(jax.random.fold_in(key, 11), pair_count)
    chosen = ranking < lagging_pairs
    member = jax.random.randint(jax.random.fold_in(key, 12), (pair_count,), 0, 2)
    index = jnp.arange(NODE_NUMBER, dtype=jnp.int32)
    pair_of = index // 2
    lagging_workers = jnp.logical_and(chosen[pair_of], index % 2 == member[pair_of])
    listed_points = jnp.nonzero(jnp.logical_not(lagging_workers), size=SURV)[0].astype(jnp.int32)
    return (listed_points, lagging_workers)


def draw_responding_nodes(key, part):
    listed_points, lagging_workers = remaining_points(key)
    return listed_points


def draw_second_operand_encoded(key, part):
    quarter = INNER // 4
    half = COLS // 2
    listed_points, lagging_workers = remaining_points(key)
    blocks = jax.random.truncated_normal(jax.random.fold_in(key, 21), -4.0, 4.0, (4, 2, quarter, half), jnp.float32) / math.sqrt(INNER)
    exponent = (3.0 - jnp.arange(4, dtype=jnp.float32))[:, None] + 4.0 * jnp.arange(2, dtype=jnp.float32)[None, :]
    stale_exponent = (3.0 - jnp.arange(4, dtype=jnp.float32))[:, None] + 4.0 * (1.0 - jnp.arange(2, dtype=jnp.float32))[None, :]

    def one_point(point):
        angle = 2.0 * math.pi * point.astype(jnp.float32) / NODE_NUMBER
        stale = lagging_workers[point].astype(jnp.float32) * 0.5
        multiplier_actual = jnp.cos(angle * exponent) + stale * jnp.cos(angle * stale_exponent)
        multiplier_image = jnp.sin(angle * exponent) + stale * jnp.sin(angle * stale_exponent)
        coef = jnp.stack([multiplier_actual, multiplier_image], axis=0)
        share = jnp.einsum('klqn,ckl->qcn', blocks, coef, precision=lax.Precision.HIGHEST)
        return jnp.clip(share, -0.5, 0.5).astype(jnp.bfloat16)
    return lax.map(one_point, jnp.arange(NODE_NUMBER, dtype=jnp.int32))


def block_scale(key, extent, cuts, least, high):
    gain = 1.0
    for dim, blocks in cuts:
        heights = jax.random.uniform(jax.random.fold_in(jax.random.fold_in(key, 6), dim), (blocks,), jnp.float32, least / len(cuts), high / len(cuts))
        gain = gain * jnp.repeat(jnp.exp(heights), extent[dim] // blocks).reshape((-1,) + (1,) * (len(extent) - 1 - dim))
    return gain


def centred(rng, shape, scale, most, pieces=(), kind=jnp.bfloat16):
    factor_of = block_scale(rng, shape, pieces, -0.22, 0.18) if pieces else 1.0
    values = jax.random.normal(rng, shape, jnp.float32) * scale * factor_of
    return jnp.minimum(jnp.maximum(values, -most), most).astype(kind)


def setup_inputs(seed: int = 0) -> dict:
    key_of = jax.random.split(jax.random.key(seed), 4)
    source_matrix_tiles = centred(key_of[0], (2, ROWS_HALF, 4, INNER // 4), 1.0, 6.0, ((1, 16), (3, 32)))
    second_operand_encoded = draw_second_operand_encoded(jax.random.fold_in(key_of[3], 71), 0)
    responding_nodes = draw_responding_nodes(jax.random.fold_in(key_of[3], 71), 0)
    return {"source_matrix_tiles": source_matrix_tiles, "second_operand_encoded": second_operand_encoded, "responding_nodes": responding_nodes}


TWO_PI_RADIANS = 2.0 * math.pi


def point_trig(node_phases):
    exponent = jnp.arange(4, dtype=jnp.float32)[None, :] + 8.0 * jnp.arange(2, dtype=jnp.float32)[:, None]
    phase = node_phases[:, None, None] * exponent[None]
    return jnp.stack([jnp.cos(phase), jnp.sin(phase)], axis=1)


def recovery_coefficients(responding_nodes):
    responder_number = responding_nodes.shape[0]
    grid_index = jnp.arange(NODE_NUMBER, dtype=jnp.int32)
    grid_angle = TWO_PI_RADIANS * grid_index.astype(jnp.float32) / NODE_NUMBER
    node_angle = TWO_PI_RADIANS * responding_nodes.astype(jnp.float32) / NODE_NUMBER
    diff_real = jnp.cos(grid_angle)[None, :] - jnp.cos(node_angle)[:, None]
    diff_imag = jnp.sin(grid_angle)[None, :] - jnp.sin(node_angle)[:, None]
    ranks = jnp.arange(responder_number, dtype=jnp.int32)
    itself = (ranks[:, None] == ranks[None, :])[:, :, None]
    factor_real = jnp.where(itself, jnp.float32(1.0), diff_real[None])
    factor_imag = jnp.where(itself, jnp.float32(0.0), diff_imag[None])
    padded_width = 1 << (responder_number - 1).bit_length()
    extra = padded_width - responder_number
    factor_real = jnp.concatenate(
        [factor_real, jnp.ones((responder_number, extra, NODE_NUMBER), jnp.float32)], axis=1)
    factor_imag = jnp.concatenate(
        [factor_imag, jnp.zeros((responder_number, extra, NODE_NUMBER), jnp.float32)], axis=1)
    while factor_real.shape[1] > 1:
        middle = factor_real.shape[1] // 2
        left_real, right_real = factor_real[:, :middle], factor_real[:, middle:]
        left_imag, right_imag = factor_imag[:, :middle], factor_imag[:, middle:]
        factor_real = left_real * right_real - left_imag * right_imag
        factor_imag = left_real * right_imag + left_imag * right_real
    sample_real = factor_real[:, 0]
    sample_imag = factor_imag[:, 0]
    wanted = 3.0 + 4.0 * jnp.arange(4, dtype=jnp.float32)
    table_angle = -grid_angle[:, None] * wanted[None, :]
    table_cos = jnp.cos(table_angle)
    table_sin = jnp.sin(table_angle)
    highest = lax.Precision.HIGHEST
    numer_real = (jnp.dot(sample_real, table_cos, precision=highest) - jnp.dot(sample_imag, table_sin, precision=highest)) / NODE_NUMBER
    numer_imag = (jnp.dot(sample_real, table_sin, precision=highest) + jnp.dot(sample_imag, table_cos, precision=highest)) / NODE_NUMBER
    onehot = (responding_nodes[:, None] == grid_index[None, :]).astype(jnp.float32)
    denom_real = jnp.sum(onehot * sample_real, axis=1)
    denom_imag = jnp.sum(onehot * sample_imag, axis=1)
    magnitude = denom_real * denom_real + denom_imag * denom_imag
    coefficient_actual = (numer_real * denom_real[:, None] + numer_imag * denom_imag[:, None]) / magnitude[:, None]
    coefficient_image = (numer_imag * denom_real[:, None] - numer_real * denom_imag[:, None]) / magnitude[:, None]
    return coefficient_actual, coefficient_image


def reference(source_matrix_tiles, second_operand_encoded, responding_nodes):
    coefficient_actual, coefficient_image = recovery_coefficients(responding_nodes)
    rows_half = source_matrix_tiles.shape[1]
    quarter = source_matrix_tiles.shape[3]
    cols_half = second_operand_encoded.shape[3]
    a_wide = source_matrix_tiles.astype(jnp.float32)

    def gather_matrix_sum(running, inputs):
        point, real_row, imag_row = inputs
        node_phases = TWO_PI_RADIANS * point.astype(jnp.float32)[None] / NODE_NUMBER
        trig = point_trig(node_phases)[0]
        coded = jnp.einsum("irkn,cik->crn", a_wide, trig, precision=lax.Precision.HIGHEST).astype(jnp.bfloat16)
        share = lax.dynamic_index_in_dim(second_operand_encoded, point, 0, keepdims=False)
        product = jnp.dot(coded.reshape(2 * rows_half, quarter), share.reshape(quarter, 2 * cols_half),
                          preferred_element_type=jnp.float32)
        real_part = product[:rows_half, :cols_half] - product[rows_half:, cols_half:]
        imag_part = product[:rows_half, cols_half:] + product[rows_half:, :cols_half]
        term = jnp.einsum("il,rn->irln", real_row.reshape(2, 2), real_part, precision=lax.Precision.HIGHEST)
        term = term - jnp.einsum("il,rn->irln", imag_row.reshape(2, 2), imag_part, precision=lax.Precision.HIGHEST)
        return running + term, None

    starting_carry = jnp.zeros((2, rows_half, 2, cols_half), jnp.float32)
    output_matrix, ignored_element = lax.scan(gather_matrix_sum, starting_carry, (responding_nodes.astype(jnp.int32), coefficient_actual, coefficient_image))
    return output_matrix
```

```python
import math

import jax
import jax.numpy as jnp
import numpy as np
from jax import lax
from jax.experimental import pallas as pl
from jax.experimental.pallas import tpu as pltpu
from jax.sharding import Mesh
from jax.sharding import PartitionSpec as P


NODE_NUMBER = 32
PAIRS = 16
EXTRAS = 3
XS = 4
YS = 8
PANELS = XS * YS
ROWS = 384
CHUNK_ROWS = 464
INTERPRET = False

TWO_PI_RADIANS = 2.0 * math.pi


def trig_table():
    exponent = np.arange(4, dtype=np.float32)[None, :] + 8 * np.arange(2, dtype=np.float32)[:, None]
    point = np.arange(NODE_NUMBER, dtype=np.float32)
    phase = np.float32(TWO_PI_RADIANS) * point / np.float32(NODE_NUMBER)
    angle = (phase[:, None, None] * exponent[None]).astype(np.float64)
    table = np.stack([np.cos(angle), np.sin(angle)], axis=1)
    return table.reshape(NODE_NUMBER, 16).astype(np.float32)


def recovery_coefficients(responding_nodes):
    responder_number = responding_nodes.shape[0]
    grid_index = jnp.arange(NODE_NUMBER, dtype=jnp.int32)
    grid_angle = TWO_PI_RADIANS * grid_index.astype(jnp.float32) / NODE_NUMBER
    node_angle = TWO_PI_RADIANS * responding_nodes.astype(jnp.float32) / NODE_NUMBER
    diff_real = jnp.cos(grid_angle)[None, :] - jnp.cos(node_angle)[:, None]
    diff_imag = jnp.sin(grid_angle)[None, :] - jnp.sin(node_angle)[:, None]
    ranks = jnp.arange(responder_number, dtype=jnp.int32)
    itself = (ranks[:, None] == ranks[None, :])[:, :, None]
    factor_real = jnp.where(itself, jnp.float32(1.0), diff_real[None])
    factor_imag = jnp.where(itself, jnp.float32(0.0), diff_imag[None])
    padded_width = 1 << (responder_number - 1).bit_length()
    extra = padded_width - responder_number
    factor_real = jnp.concatenate(
        [factor_real, jnp.ones((responder_number, extra, NODE_NUMBER), jnp.float32)], axis=1
    )
    factor_imag = jnp.concatenate(
        [factor_imag, jnp.zeros((responder_number, extra, NODE_NUMBER), jnp.float32)], axis=1
    )
    while factor_real.shape[1] > 1:
        middle = factor_real.shape[1] // 2
        left_real, right_real = (factor_real[:, :middle], factor_real[:, middle:])
        left_imag, right_imag = (factor_imag[:, :middle], factor_imag[:, middle:])
        factor_real = left_real * right_real - left_imag * right_imag
        factor_imag = left_real * right_imag + left_imag * right_real
    sample_real = factor_real[:, 0]
    sample_imag = factor_imag[:, 0]
    wanted = 3.0 + 4.0 * jnp.arange(4, dtype=jnp.float32)
    table_angle = -grid_angle[:, None] * wanted[None, :]
    table_cos = jnp.cos(table_angle)
    table_sin = jnp.sin(table_angle)
    highest = lax.Precision.HIGHEST
    numer_real = (
        jnp.dot(sample_real, table_cos, precision=highest)
        - jnp.dot(sample_imag, table_sin, precision=highest)
    ) / NODE_NUMBER
    numer_imag = (
        jnp.dot(sample_real, table_sin, precision=highest)
        + jnp.dot(sample_imag, table_cos, precision=highest)
    ) / NODE_NUMBER
    onehot = (responding_nodes[:, None] == grid_index[None, :]).astype(jnp.float32)
    denom_real = jnp.sum(onehot * sample_real, axis=1)
    denom_imag = jnp.sum(onehot * sample_imag, axis=1)
    magnitude = denom_real * denom_real + denom_imag * denom_imag
    coefficient_actual = (
        numer_real * denom_real[:, None] + numer_imag * denom_imag[:, None]
    ) / magnitude[:, None]
    coefficient_image = (
        numer_imag * denom_real[:, None] - numer_real * denom_imag[:, None]
    ) / magnitude[:, None]
    return (coefficient_actual, coefficient_image)


def encode_kernel(main_trig, extra_trig, tiles, out, stack):
    upper = lax.broadcasted_iota(jnp.int32, (8, 128), 0) < 4

    def block(trig, at):
        top_r = trig[at] * tiles[0, :8, :]
        top_i = trig[at + 8] * tiles[0, :8, :]
        low_r = trig[at] * tiles[0, 8:, :]
        low_i = trig[at + 8] * tiles[0, 8:, :]
        for b in range(1, 8):
            top_r += trig[at + b] * tiles[b, :8, :]
            top_i += trig[at + 8 + b] * tiles[b, :8, :]
            low_r += trig[at + b] * tiles[b, 8:, :]
            low_i += trig[at + 8 + b] * tiles[b, 8:, :]
        return top_r, top_i, jnp.where(upper, low_r, low_i)

    stack[...] = jnp.zeros_like(stack)
    for e in range(EXTRAS):
        for v, tile in enumerate(block(extra_trig, 16 * e)):
            stack[24 * e + 8 * v : 24 * e + 8 * v + 8, :] = tile
    turned = stack[...].T
    for t in range(PAIRS):
        parts = list(block(main_trig, 16 * t)) + [turned[8 * t : 8 * t + 8, :]]
        out[t] = jnp.concatenate(parts, axis=0).astype(jnp.bfloat16)


def encode(main_trig, extra_trig, tiles):
    return pl.pallas_call(
        encode_kernel,
        out_shape=jax.ShapeDtypeStruct((PAIRS, 32, 128), jnp.bfloat16),
        in_specs=[
            pl.BlockSpec(memory_space=pltpu.SMEM),
            pl.BlockSpec(memory_space=pltpu.SMEM),
            pl.BlockSpec(memory_space=pltpu.VMEM),
        ],
        out_specs=pl.BlockSpec(memory_space=pltpu.VMEM),
        scratch_shapes=[pltpu.VMEM((128, 128), jnp.float32)],
        name="encode",
        interpret=INTERPRET,
    )(main_trig, extra_trig, tiles)


def compact_kernel(got, out, rows):
    lane = lax.broadcasted_iota(jnp.int32, (8, 128), 1)
    pieces = []
    for g in range(PAIRS):
        block = got[g].astype(jnp.float32)
        rows[24 * g : 24 * g + 24, :] = block[:24]
        pieces.append(block[24:])
    for e in range(EXTRAS):
        for v in range(3):
            tile = jnp.zeros((8, 128), jnp.float32)
            for g in range(PAIRS):
                start = 24 * g - 128 * v
                if start + 24 <= 0 or start >= 128:
                    continue
                moved = pltpu.roll(pieces[g], (start - 24 * e) % 128, 1)
                tile = jnp.where((lane >= start) & (lane < start + 24), moved, tile)
            at = ROWS + 8 * (3 * e + v)
            rows[at : at + 8, :] = tile
    rows[ROWS + 72 :, :] = jnp.zeros((8, 128), jnp.float32)
    out[...] = rows[...].astype(jnp.bfloat16)


def compact(got):
    return pl.pallas_call(
        compact_kernel,
        out_shape=jax.ShapeDtypeStruct((CHUNK_ROWS, 128), jnp.bfloat16),
        in_specs=[pl.BlockSpec(memory_space=pltpu.VMEM)],
        out_specs=pl.BlockSpec(memory_space=pltpu.VMEM),
        scratch_shapes=[pltpu.VMEM((CHUNK_ROWS, 128), jnp.float32)],
        name="compact",
        interpret=INTERPRET,
    )(got)


def split_pairs(pairs, scratch):
    count = pairs.shape[0] // 2
    scratch[: 2 * count, :] = pairs.astype(jnp.float32)
    real = scratch[pl.ds(0, count, stride=2), :]
    imag = scratch[pl.ds(1, count, stride=2), :]
    return jnp.concatenate([real, imag], axis=1).astype(jnp.bfloat16)


def share_kernel(picks, share, own, out, scratch):
    out[0] = split_pairs(share[0], scratch)


def split_share(picks, share, own):
    return pl.pallas_call(
        share_kernel,
        out_shape=jax.ShapeDtypeStruct((XS, 1024, 256), jnp.bfloat16),
        grid_spec=pltpu.PrefetchScalarGridSpec(
            num_scalar_prefetch=1,
            grid=(XS,),
            in_specs=[
                pl.BlockSpec((1, 2048, 128), lambda k, picks: (picks[0], k, 0)),
                pl.BlockSpec(memory_space=pl.ANY),
            ],
            out_specs=pl.BlockSpec((1, 1024, 256), lambda k, picks: (k, 0, 0)),
            scratch_shapes=[pltpu.VMEM((2048, 128), jnp.float32)],
        ),
        name="split_share",
        cost_estimate=pl.CostEstimate(flops=400_000_000, bytes_accessed=4_200_000, transcendentals=0),
        interpret=INTERPRET,
    )(picks, share, own)


def wide(chunk, first, count):
    return jnp.concatenate([chunk[first + y, :ROWS, :] for y in range(count)], axis=1)


def product_kernel(
    picks, weights, share, spread, own, right, left, far_a, far_b, out, acc, extra, acc_extra, scratch
):
    def dot(a, b):
        return jnp.dot(a, b, preferred_element_type=jnp.float32)

    acc[...] = dot(wide(own, 0, YS), share[picks[1]])
    acc[...] += dot(wide(right, 0, YS), share[picks[2]])
    acc[...] += dot(wide(left, 0, YS), share[picks[3]])
    acc[...] += dot(wide(far_a, 0, YS // 2), share[picks[4], :512, :])
    acc[...] += dot(wide(far_b, 0, YS // 2), share[picks[4], 512:, :])

    def place(chunk, count, panel):
        for y in range(count):
            rows = chunk[y, ROWS:, :].astype(jnp.float32)
            at = pl.multiple_of(8 * (panel + y), 8)
            for v in range(9):
                extra[pl.ds(at, 8), 128 * v : 128 * v + 128] = rows[8 * v : 8 * v + 8]

    place(own, YS, YS * picks[1])
    place(right, YS, YS * picks[2])
    place(left, YS, YS * picks[3])
    place(far_a, YS // 2, YS * picks[4])
    place(far_b, YS // 2, YS * picks[4] + YS // 2)
    for e in range(EXTRAS):
        slices = split_pairs(spread[picks[5 + e]], scratch)
        turned = extra[:, ROWS * e : ROWS * e + ROWS].astype(jnp.bfloat16)
        acc_extra[e] = lax.dot_general(
            turned, slices, (((0,), (0,)), ((), ())), preferred_element_type=jnp.float32
        )

    upper = lax.broadcasted_iota(jnp.int32, (8, 128), 0) < 4

    def decode(g, carry):
        top = [jnp.zeros((8, 128), jnp.float32)] * 4
        low = [jnp.zeros((8, 128), jnp.float32)] * 4
        at = pl.multiple_of(24 * g, 8)
        for s in range(1 + EXTRAS):
            tiles = [
                acc[pl.ds(at + 8 * v, 8), :] if s == 0 else acc_extra[s - 1, pl.ds(at + 8 * v, 8), :]
                for v in range(3)
            ]
            top_r = tiles[0][:, :128] - tiles[1][:, 128:]
            top_i = tiles[0][:, 128:] + tiles[1][:, :128]
            low_r = tiles[2][:, :128] - pltpu.roll(tiles[2][:, 128:], 4, 0)
            low_i = tiles[2][:, 128:] + pltpu.roll(tiles[2][:, :128], 4, 0)
            for b in range(4):
                w_r = weights[8 * s + b]
                w_i = weights[8 * s + 4 + b]
                top[b] = top[b] + (w_r * top_r - w_i * top_i)
                low[b] = low[b] + (w_r * low_r - w_i * low_i)
        low_a = jnp.where(upper, low[0], pltpu.roll(low[1], 4, 0))
        low_b = jnp.where(upper, low[2], pltpu.roll(low[3], 4, 0))
        out[g] = jnp.concatenate(top + [low_a, low_b], axis=0)
        return carry

    lax.fori_loop(0, PAIRS, decode, 0)


def product(picks, weights, share, spread, own, right, left, far_a, far_b):
    return pl.pallas_call(
        product_kernel,
        out_shape=jax.ShapeDtypeStruct((PAIRS, 48, 128), jnp.float32),
        in_specs=[pl.BlockSpec(memory_space=pltpu.SMEM)] * 2 + [pl.BlockSpec(memory_space=pltpu.VMEM)] * 7,
        out_specs=pl.BlockSpec(memory_space=pltpu.VMEM),
        scratch_shapes=[
            pltpu.VMEM((ROWS, 256), jnp.float32),
            pltpu.VMEM((256, 1152), jnp.float32),
            pltpu.VMEM((EXTRAS, ROWS, 256), jnp.float32),
            pltpu.VMEM((512, 128), jnp.float32),
        ],
        name="product",
        interpret=INTERPRET,
    )(picks, weights, share, spread, own, right, left, far_a, far_b)


def choose(responding_nodes):
    listed = jnp.any(
        responding_nodes[:, None] == jnp.arange(NODE_NUMBER, dtype=jnp.int32)[None, :], axis=0
    ).reshape(PAIRS, 2)
    both = listed[:, 0] & listed[:, 1]
    index = jnp.arange(PAIRS, dtype=jnp.int32)
    before = jnp.sum((index[None, :] < index[:, None]) & both[None, :], axis=1)
    extra_pair = both[None, :] & (before[None, :] == jnp.arange(EXTRAS, dtype=jnp.int32)[:, None])
    return listed[:, 0], extra_pair


def source_tiles(source):
    blocks = source.astype(jnp.float32).transpose(0, 2, 1, 3).reshape(8, 12, 128)
    return jnp.concatenate([blocks, blocks[:, 8:]], axis=1)


def summed(received):
    total = jnp.sum(received, axis=0)
    top = total[:32].reshape(2, 2, 8, 128)
    low = total[32:].reshape(2, 2, 4, 128)
    return jnp.concatenate([top, low], axis=2).transpose(0, 2, 1, 3)


def shards(source_matrix_tiles, second_operand_encoded, responding_nodes):
    table = jnp.asarray(trig_table())
    even_listed, extra_pair = choose(responding_nodes)
    pair_table = table.reshape(PAIRS, 2, 16)
    main_trig = jnp.where(even_listed[:, None], pair_table[:, 0], pair_table[:, 1])
    extra_trig = jnp.sum(jnp.where(extra_pair[:, :, None], pair_table[None, :, 1], 0.0), axis=1)
    sent = encode(main_trig.reshape(-1), extra_trig.reshape(-1), source_tiles(source_matrix_tiles))
    got = lax.all_to_all(sent, "group", split_axis=0, concat_axis=0, tiled=True)

    odd = second_operand_encoded[1].reshape(PANELS, PAIRS, 8, 2, 128).transpose(1, 0, 2, 3, 4)
    odd, got = lax.optimization_barrier((odd, got))
    spread = lax.all_to_all(odd, "group", split_axis=0, concat_axis=0, tiled=True)
    own = lax.all_gather(compact(got), "y")

    responding_nodes, own = lax.optimization_barrier((responding_nodes, own))
    right = lax.ppermute(own, "x", [(i, (i + 1) % XS) for i in range(XS)])
    left = lax.ppermute(own, "x", [(i, (i - 1) % XS) for i in range(XS)])
    far_a = lax.ppermute(right[: YS // 2], "x", [(i, (i + 1) % XS) for i in range(XS)])
    far_b = lax.ppermute(left[YS // 2 :], "x", [(i, (i - 1) % XS) for i in range(XS)])

    coefficient_actual, coefficient_image = recovery_coefficients(responding_nodes)
    even_listed, extra_pair = choose(responding_nodes)
    group = lax.axis_index("group")
    x = lax.axis_index("x")
    second = jnp.where(even_listed[group], 0, 1).astype(jnp.int32)
    extra_group = jnp.sum(
        jnp.where(extra_pair, jnp.arange(PAIRS, dtype=jnp.int32)[None, :], 0), axis=1
    ).astype(jnp.int32)
    used = jnp.concatenate([(2 * group + second)[None], 2 * extra_group + 1])
    point_selector = (used[:, None] == responding_nodes[None, :])[:, :, None]
    weights = jnp.concatenate(
        [
            jnp.sum(jnp.where(point_selector, coefficient_actual[None], 0.0), axis=1),
            jnp.sum(jnp.where(point_selector, coefficient_image[None], 0.0), axis=1),
        ],
        axis=1,
    ).reshape(-1)
    panels = jnp.stack([x, (x - 1) % XS, (x + 1) % XS, (x + 2) % XS]).astype(jnp.int32)
    picks = jnp.concatenate([second[None], panels, extra_group])

    share = split_share(picks, second_operand_encoded.reshape(2, 8192, 128), own)
    partial = product(
        picks, weights, share, spread.reshape(PAIRS, 512, 128), own, right, left, far_a, far_b
    )
    received = lax.all_to_all(partial, "group", split_axis=0, concat_axis=0, tiled=True)
    return summed(received)


def solution(mesh):
    torus = Mesh(mesh.devices.reshape(mesh.shape["group"], XS, YS), ("group", "x", "y"))
    return jax.shard_map(
        shards,
        mesh=torus,
        in_specs=(P(None, "group", None, ("x", "y")), P("group", None, None, ("x", "y")), P()),
        out_specs=P(None, "group", None, ("x", "y")),
        check_vma=False,
    )
```

```python
import math

import jax
import jax.numpy as jnp
import numpy as np
from jax import lax
from jax.experimental import pallas as pl
from jax.experimental.pallas import tpu as pltpu
from jax.sharding import Mesh
from jax.sharding import PartitionSpec as P


NODE_NUMBER = 32
PAIRS = 16
EXTRAS = 3
XS = 4
YS = 8
QUADS = YS // 2
PANELS = XS * YS
ROWS = 384
CHUNK_ROWS = 464
INTERPRET = False

TWO_PI_RADIANS = 2.0 * math.pi


def trig_table():
    exponent = np.arange(4, dtype=np.float32)[None, :] + 8 * np.arange(2, dtype=np.float32)[:, None]
    point = np.arange(NODE_NUMBER, dtype=np.float32)
    phase = np.float32(TWO_PI_RADIANS) * point / np.float32(NODE_NUMBER)
    angle = (phase[:, None, None] * exponent[None]).astype(np.float64)
    table = np.stack([np.cos(angle), np.sin(angle)], axis=1)
    return table.reshape(NODE_NUMBER, 16).astype(np.float32)


def recovery_coefficients(responding_nodes):
    responder_number = responding_nodes.shape[0]
    grid_index = jnp.arange(NODE_NUMBER, dtype=jnp.int32)
    grid_angle = TWO_PI_RADIANS * grid_index.astype(jnp.float32) / NODE_NUMBER
    node_angle = TWO_PI_RADIANS * responding_nodes.astype(jnp.float32) / NODE_NUMBER
    diff_real = jnp.cos(grid_angle)[None, :] - jnp.cos(node_angle)[:, None]
    diff_imag = jnp.sin(grid_angle)[None, :] - jnp.sin(node_angle)[:, None]
    ranks = jnp.arange(responder_number, dtype=jnp.int32)
    itself = (ranks[:, None] == ranks[None, :])[:, :, None]
    factor_real = jnp.where(itself, jnp.float32(1.0), diff_real[None])
    factor_imag = jnp.where(itself, jnp.float32(0.0), diff_imag[None])
    padded_width = 1 << (responder_number - 1).bit_length()
    extra = padded_width - responder_number
    factor_real = jnp.concatenate(
        [factor_real, jnp.ones((responder_number, extra, NODE_NUMBER), jnp.float32)], axis=1
    )
    factor_imag = jnp.concatenate(
        [factor_imag, jnp.zeros((responder_number, extra, NODE_NUMBER), jnp.float32)], axis=1
    )
    while factor_real.shape[1] > 1:
        middle = factor_real.shape[1] // 2
        left_real, right_real = (factor_real[:, :middle], factor_real[:, middle:])
        left_imag, right_imag = (factor_imag[:, :middle], factor_imag[:, middle:])
        factor_real = left_real * right_real - left_imag * right_imag
        factor_imag = left_real * right_imag + left_imag * right_real
    sample_real = factor_real[:, 0]
    sample_imag = factor_imag[:, 0]
    wanted = 3.0 + 4.0 * jnp.arange(4, dtype=jnp.float32)
    table_angle = -grid_angle[:, None] * wanted[None, :]
    table_cos = jnp.cos(table_angle)
    table_sin = jnp.sin(table_angle)
    highest = lax.Precision.HIGHEST
    numer_real = (
        jnp.dot(sample_real, table_cos, precision=highest)
        - jnp.dot(sample_imag, table_sin, precision=highest)
    ) / NODE_NUMBER
    numer_imag = (
        jnp.dot(sample_real, table_sin, precision=highest)
        + jnp.dot(sample_imag, table_cos, precision=highest)
    ) / NODE_NUMBER
    onehot = (responding_nodes[:, None] == grid_index[None, :]).astype(jnp.float32)
    denom_real = jnp.sum(onehot * sample_real, axis=1)
    denom_imag = jnp.sum(onehot * sample_imag, axis=1)
    magnitude = denom_real * denom_real + denom_imag * denom_imag
    coefficient_actual = (
        numer_real * denom_real[:, None] + numer_imag * denom_imag[:, None]
    ) / magnitude[:, None]
    coefficient_image = (
        numer_imag * denom_real[:, None] - numer_real * denom_imag[:, None]
    ) / magnitude[:, None]
    return (coefficient_actual, coefficient_image)


def encode_kernel(nodes, table, source, out, flags, extra_points, rows, stack):
    for j in range(NODE_NUMBER):
        flags[j] = 0
    for s in range(nodes.shape[0]):
        flags[nodes[s]] = 1
    found = jnp.int32(0)
    for g in range(PAIRS):
        extra_points[found] = 2 * g + 1
        found = found + flags[2 * g] * flags[2 * g + 1]

    rows[...] = source[...].astype(jnp.float32)
    tops = []
    lows = []
    for b in range(8):
        at = 48 * (b // 4) + b % 4
        tops.append(rows[pl.ds(at, 8, stride=4), :])
        low = rows[pl.ds(at + 32, 4, stride=4), :]
        lows.append(jnp.concatenate([low, low], axis=0))
    upper = lax.broadcasted_iota(jnp.int32, (8, 128), 0) < 4

    def block(point):
        at = 16 * point
        real = [table[at + b] for b in range(8)]
        imag = [table[at + 8 + b] for b in range(8)]
        top_r = sum(real[b] * tops[b] for b in range(8))
        top_i = sum(imag[b] * tops[b] for b in range(8))
        low = sum(jnp.where(upper, real[b], imag[b]) * lows[b] for b in range(8))
        return [top_r, top_i, low]

    stack[...] = jnp.zeros_like(stack)
    for e in range(EXTRAS):
        for v, tile in enumerate(block(extra_points[e])):
            stack[24 * e + 8 * v : 24 * e + 8 * v + 8, :] = tile
    stack[...] = stack[...].T

    def main(t, carry):
        parts = block(2 * t + 1 - flags[2 * t])
        parts.append(stack[pl.ds(pl.multiple_of(8 * t, 8), 8), :])
        value = jnp.concatenate(parts, axis=0).astype(jnp.bfloat16)
        for q in range(QUADS):
            out[t, q] = value
        return carry

    lax.fori_loop(0, PAIRS, main, 0)


def encode(nodes, table, source):
    return pl.pallas_call(
        encode_kernel,
        out_shape=jax.ShapeDtypeStruct((PAIRS, QUADS, 32, 128), jnp.bfloat16),
        in_specs=[
            pl.BlockSpec(memory_space=pltpu.SMEM),
            pl.BlockSpec(memory_space=pltpu.SMEM),
            pl.BlockSpec(memory_space=pltpu.VMEM),
        ],
        out_specs=pl.BlockSpec(memory_space=pltpu.VMEM),
        scratch_shapes=[
            pltpu.SMEM((NODE_NUMBER,), jnp.int32),
            pltpu.SMEM((PAIRS,), jnp.int32),
            pltpu.VMEM((96, 128), jnp.float32),
            pltpu.VMEM((128, 128), jnp.float32),
        ],
        name="encode",
        interpret=INTERPRET,
    )(nodes, table, source)


def compact_kernel(got, out, rows):
    lane = lax.broadcasted_iota(jnp.int32, (8, 128), 1)
    rows[ROWS + 72 :, :] = jnp.zeros((8, 128), jnp.float32)

    def one(q, carry):
        pieces = []
        for g in range(PAIRS):
            block = got[QUADS * g + q].astype(jnp.float32)
            rows[24 * g : 24 * g + 24, :] = block[:24]
            pieces.append(block[24:])
        for e in range(EXTRAS):
            for v in range(3):
                tile = jnp.zeros((8, 128), jnp.float32)
                for g in range(PAIRS):
                    start = 24 * g - 128 * v
                    if start + 24 <= 0 or start >= 128:
                        continue
                    moved = pltpu.roll(pieces[g], (start - 24 * e) % 128, 1)
                    tile = jnp.where((lane >= start) & (lane < start + 24), moved, tile)
                at = ROWS + 8 * (3 * e + v)
                rows[at : at + 8, :] = tile
        out[q] = rows[...].astype(jnp.bfloat16)
        return carry

    lax.fori_loop(0, QUADS, one, 0)


def compact(got):
    return pl.pallas_call(
        compact_kernel,
        out_shape=jax.ShapeDtypeStruct((QUADS, CHUNK_ROWS, 128), jnp.bfloat16),
        in_specs=[pl.BlockSpec(memory_space=pltpu.VMEM)],
        out_specs=pl.BlockSpec(memory_space=pltpu.VMEM),
        scratch_shapes=[pltpu.VMEM((CHUNK_ROWS, 128), jnp.float32)],
        name="compact",
        interpret=INTERPRET,
    )(got)


def split_pairs(pairs, scratch):
    count = pairs.shape[0] // 2
    scratch[: 2 * count, :] = pairs.astype(jnp.float32)
    real = scratch[pl.ds(0, count, stride=2), :]
    imag = scratch[pl.ds(1, count, stride=2), :]
    return jnp.concatenate([real, imag], axis=1).astype(jnp.bfloat16)


def share_kernel(picks, share, out, scratch):
    for y in range(YS):
        piece = split_pairs(share[0, 256 * y : 256 * y + 256, :], scratch)
        out[0, y % 2, 128 * (y // 2) : 128 * (y // 2) + 128, :] = piece


def split_share(picks, share):
    return pl.pallas_call(
        share_kernel,
        out_shape=jax.ShapeDtypeStruct((XS, 2, 512, 256), jnp.bfloat16),
        grid_spec=pltpu.PrefetchScalarGridSpec(
            num_scalar_prefetch=1,
            grid=(XS,),
            in_specs=[pl.BlockSpec((1, 2048, 128), lambda k, picks: (picks[0], k, 0))],
            out_specs=pl.BlockSpec((1, 2, 512, 256), lambda k, picks: (k, 0, 0, 0)),
            scratch_shapes=[pltpu.VMEM((256, 128), jnp.float32)],
        ),
        name="split_share",
        cost_estimate=pl.CostEstimate(flops=400_000_000, bytes_accessed=4_200_000, transcendentals=0),
        interpret=INTERPRET,
    )(picks, share)


def wide(chunk):
    return jnp.concatenate([chunk[q, :ROWS, :] for q in range(QUADS)], axis=1)


def dot(a, b):
    return jnp.dot(a, b, preferred_element_type=jnp.float32)


EARLY = ((0, True), (0, False), (-1, True), (1, True))
LATE = ((-1, False), (1, False), (2, True), (2, False))


def block_of(picks, kind):
    offset, same = kind
    x = (picks[1] + offset + XS) % XS
    return x, picks[2] if same else 1 - picks[2]


def early_kernel(picks, share, a, b, right_a, left_a, acc):
    for n, (chunk, kind) in enumerate(zip((a, b, right_a, left_a), EARLY)):
        x, parity = block_of(picks, kind)
        term = dot(wide(chunk), share[x, parity])
        if n == 0:
            acc[...] = term
        else:
            acc[...] += term


def early_product(picks, share, chunks):
    return pl.pallas_call(
        early_kernel,
        out_shape=jax.ShapeDtypeStruct((ROWS, 256), jnp.float32),
        in_specs=[pl.BlockSpec(memory_space=pltpu.SMEM)] + [pl.BlockSpec(memory_space=pltpu.VMEM)] * 5,
        out_specs=pl.BlockSpec(memory_space=pltpu.VMEM),
        name="early_product",
        cost_estimate=pl.CostEstimate(flops=400_000_000, bytes_accessed=4_200_000, transcendentals=0),
        interpret=INTERPRET,
    )(picks, share, *chunks)


def late_kernel(
    picks, weights, share, spread, before, c0, c1, c2, c3, c4, c5, c6, c7, out,
    acc, blocks, small, ends, late, extra, acc_extra, scratch, sems,
):
    early = (c0, c1, c2, c3)
    chunks = (c4, c5, c6, c7)
    copies = []

    def start(source, target):
        copy = pltpu.make_async_copy(source, target, sems.at[len(copies)])
        copy.start()
        copies.append(copy)

    start(spread, small)
    for n in range(4):
        start(early[n].at[:, pl.ds(ROWS, 80), :], ends.at[n])
    for n in range(4):
        x, parity = block_of(picks, LATE[n])
        start(chunks[n], late.at[n])
        start(share.at[x, parity], blocks.at[n])
    start(before, acc)

    def place(rows_of, kind):
        x, parity = block_of(picks, kind)
        for q in range(QUADS):
            rows = rows_of(q)
            at = pl.multiple_of(8 * (YS * x + 2 * q + parity), 8)
            for v in range(9):
                extra[pl.ds(at, 8), 128 * v : 128 * v + 128] = rows[8 * v : 8 * v + 8]

    for copy in copies[:5]:
        copy.wait()
    for n in range(4):
        place(lambda q: ends[n, q].astype(jnp.float32), EARLY[n])
    slices = [split_pairs(small[e], scratch) for e in range(EXTRAS)]
    for n in range(4):
        copies[5 + 2 * n].wait()
        place(lambda q: late[n, q, ROWS:, :].astype(jnp.float32), LATE[n])
    for e in range(EXTRAS):
        turned = extra[:, ROWS * e : ROWS * e + ROWS].astype(jnp.bfloat16)
        acc_extra[e] = lax.dot_general(
            turned, slices[e], (((0,), (0,)), ((), ())), preferred_element_type=jnp.float32
        )
    copies[13].wait()
    for n in range(4):
        copies[6 + 2 * n].wait()
        acc[...] += dot(wide(late.at[n]), blocks[n])

    upper = lax.broadcasted_iota(jnp.int32, (8, 128), 0) < 4

    def decode(g, carry):
        top = [jnp.zeros((8, 128), jnp.float32)] * 4
        low = [jnp.zeros((8, 128), jnp.float32)] * 4
        at = pl.multiple_of(24 * g, 8)
        for s in range(1 + EXTRAS):
            tiles = [
                acc[pl.ds(at + 8 * v, 8), :] if s == 0 else acc_extra[s - 1, pl.ds(at + 8 * v, 8), :]
                for v in range(3)
            ]
            top_r = tiles[0][:, :128] - tiles[1][:, 128:]
            top_i = tiles[0][:, 128:] + tiles[1][:, :128]
            low_r = tiles[2][:, :128] - pltpu.roll(tiles[2][:, 128:], 4, 0)
            low_i = tiles[2][:, 128:] + pltpu.roll(tiles[2][:, :128], 4, 0)
            for b in range(4):
                w_r = weights[8 * s + b]
                w_i = weights[8 * s + 4 + b]
                top[b] = top[b] + (w_r * top_r - w_i * top_i)
                low[b] = low[b] + (w_r * low_r - w_i * low_i)
        low_a = jnp.where(upper, low[0], pltpu.roll(low[1], 4, 0))
        low_b = jnp.where(upper, low[2], pltpu.roll(low[3], 4, 0))
        out[g] = jnp.concatenate(top + [low_a, low_b], axis=0)
        return carry

    lax.fori_loop(0, PAIRS, decode, 0)


def late_product(picks, weights, share, spread, before, early, late):
    return pl.pallas_call(
        late_kernel,
        out_shape=jax.ShapeDtypeStruct((PAIRS, 48, 128), jnp.float32),
        in_specs=[pl.BlockSpec(memory_space=pltpu.SMEM)] * 2 + [pl.BlockSpec(memory_space=pl.ANY)] * 11,
        out_specs=pl.BlockSpec(memory_space=pltpu.VMEM),
        scratch_shapes=[
            pltpu.VMEM((ROWS, 256), jnp.float32),
            pltpu.VMEM((4, 512, 256), jnp.bfloat16),
            pltpu.VMEM((EXTRAS, 512, 128), jnp.bfloat16),
            pltpu.VMEM((4, QUADS, 80, 128), jnp.bfloat16),
            pltpu.VMEM((4, QUADS, CHUNK_ROWS, 128), jnp.bfloat16),
            pltpu.VMEM((256, 1152), jnp.float32),
            pltpu.VMEM((EXTRAS, ROWS, 256), jnp.float32),
            pltpu.VMEM((512, 128), jnp.float32),
            pltpu.SemaphoreType.DMA((14,)),
        ],
        name="late_product",
        interpret=INTERPRET,
    )(picks, weights, share, spread, before, *early, *late)


def choose(responding_nodes):
    listed = jnp.any(
        responding_nodes[:, None] == jnp.arange(NODE_NUMBER, dtype=jnp.int32)[None, :], axis=0
    ).reshape(PAIRS, 2)
    both = listed[:, 0] & listed[:, 1]
    index = jnp.arange(PAIRS, dtype=jnp.int32)
    before = jnp.sum((index[None, :] < index[:, None]) & both[None, :], axis=1)
    extra_pair = both[None, :] & (before[None, :] == jnp.arange(EXTRAS, dtype=jnp.int32)[:, None])
    return listed[:, 0], extra_pair


def summed(received):
    total = jnp.sum(received, axis=0)
    top = total[:32].reshape(2, 2, 8, 128)
    low = total[32:].reshape(2, 2, 4, 128)
    return jnp.concatenate([top, low], axis=2).transpose(0, 2, 1, 3)


def shards(source_matrix_tiles, second_operand_encoded, responding_nodes):
    sent = encode(
        responding_nodes, jnp.asarray(trig_table().reshape(-1)), source_matrix_tiles.reshape(96, 128)
    ).reshape(PAIRS * QUADS, 32, 128)
    got = lax.all_to_all(sent, ("group", "quad"), split_axis=0, concat_axis=0, tiled=True)

    odd = second_operand_encoded[1].reshape(PANELS, PAIRS, 8, 2, 128).transpose(1, 0, 2, 3, 4)
    spread = lax.all_to_all(odd, "group", split_axis=0, concat_axis=0, tiled=True)
    even_listed, _ = choose(responding_nodes)
    group = lax.axis_index("group")
    second = jnp.where(even_listed[group], 0, 1).astype(jnp.int32)
    picks = jnp.stack([second, lax.axis_index("x"), lax.axis_index("parity")]).astype(jnp.int32)
    share = split_share(picks, second_operand_encoded.reshape(2, 8192, 128))
    a = compact(got)

    def shift(chunk, by):
        return lax.ppermute(chunk, "x", [(i, (i + by) % XS) for i in range(XS)])

    responding_nodes, a = lax.optimization_barrier((responding_nodes, a))
    b = lax.ppermute(a, "parity", [(0, 1), (1, 0)])
    right_a, left_a = shift(a, 1), shift(a, -1)
    right_b, left_b = shift(b, 1), shift(b, -1)
    far_a, far_b = shift(right_a, 1), shift(left_b, -1)

    coefficient_actual, coefficient_image = recovery_coefficients(responding_nodes)
    _, extra_pair = choose(responding_nodes)
    extra_group = jnp.sum(
        jnp.where(extra_pair, jnp.arange(PAIRS, dtype=jnp.int32)[None, :], 0), axis=1
    ).astype(jnp.int32)
    used = jnp.concatenate([(2 * group + second)[None], 2 * extra_group + 1])
    point_selector = (used[:, None] == responding_nodes[None, :])[:, :, None]
    weights = jnp.concatenate(
        [
            jnp.sum(jnp.where(point_selector, coefficient_actual[None], 0.0), axis=1),
            jnp.sum(jnp.where(point_selector, coefficient_image[None], 0.0), axis=1),
        ],
        axis=1,
    ).reshape(-1)

    early = (a, b, right_a, left_a)
    before = early_product(picks, share, early)
    three = jnp.stack(
        [lax.dynamic_index_in_dim(spread, extra_group[e], 0, keepdims=False) for e in range(EXTRAS)]
    ).reshape(EXTRAS, 512, 128)
    partial = late_product(
        picks, weights, share, three, before, early, (right_b, left_b, far_a, far_b)
    )
    received = lax.all_to_all(partial, "group", split_axis=0, concat_axis=0, tiled=True)
    return summed(received)


def solution(mesh):
    torus = Mesh(
        mesh.devices.reshape(mesh.shape["group"], XS, QUADS, 2), ("group", "x", "quad", "parity")
    )
    panel = ("x", "quad", "parity")
    return jax.shard_map(
        shards,
        mesh=torus,
        in_specs=(P(None, "group", None, panel), P("group", None, None, panel), P()),
        out_specs=P(None, "group", None, panel),
        check_vma=False,
    )
```

```python
import math

import jax
import jax.numpy as jnp
import numpy as np
from jax import lax
from jax.experimental import pallas as pl
from jax.experimental.pallas import tpu as pltpu
from jax.sharding import Mesh
from jax.sharding import PartitionSpec as P


NODE_NUMBER = 32
PAIRS = 16
EXTRAS = 3
XS = 4
YS = 8
QUADS = YS // 2
PANELS = XS * YS
ROWS = 384
CHUNK_ROWS = 464
INTERPRET = False

TWO_PI_RADIANS = 2.0 * math.pi


def trig_table():
    exponent = np.arange(4, dtype=np.float32)[None, :] + 8 * np.arange(2, dtype=np.float32)[:, None]
    point = np.arange(NODE_NUMBER, dtype=np.float32)
    phase = np.float32(TWO_PI_RADIANS) * point / np.float32(NODE_NUMBER)
    angle = (phase[:, None, None] * exponent[None]).astype(np.float64)
    table = np.stack([np.cos(angle), np.sin(angle)], axis=1)
    return table.reshape(NODE_NUMBER, 16).astype(np.float32)


def recovery_coefficients(responding_nodes):
    responder_number = responding_nodes.shape[0]
    grid_index = jnp.arange(NODE_NUMBER, dtype=jnp.int32)
    grid_angle = TWO_PI_RADIANS * grid_index.astype(jnp.float32) / NODE_NUMBER
    node_angle = TWO_PI_RADIANS * responding_nodes.astype(jnp.float32) / NODE_NUMBER
    diff_real = jnp.cos(grid_angle)[None, :] - jnp.cos(node_angle)[:, None]
    diff_imag = jnp.sin(grid_angle)[None, :] - jnp.sin(node_angle)[:, None]
    ranks = jnp.arange(responder_number, dtype=jnp.int32)
    itself = (ranks[:, None] == ranks[None, :])[:, :, None]
    factor_real = jnp.where(itself, jnp.float32(1.0), diff_real[None])
    factor_imag = jnp.where(itself, jnp.float32(0.0), diff_imag[None])
    padded_width = 1 << (responder_number - 1).bit_length()
    extra = padded_width - responder_number
    factor_real = jnp.concatenate(
        [factor_real, jnp.ones((responder_number, extra, NODE_NUMBER), jnp.float32)], axis=1
    )
    factor_imag = jnp.concatenate(
        [factor_imag, jnp.zeros((responder_number, extra, NODE_NUMBER), jnp.float32)], axis=1
    )
    while factor_real.shape[1] > 1:
        middle = factor_real.shape[1] // 2
        left_real, right_real = (factor_real[:, :middle], factor_real[:, middle:])
        left_imag, right_imag = (factor_imag[:, :middle], factor_imag[:, middle:])
        factor_real = left_real * right_real - left_imag * right_imag
        factor_imag = left_real * right_imag + left_imag * right_real
    sample_real = factor_real[:, 0]
    sample_imag = factor_imag[:, 0]
    wanted = 3.0 + 4.0 * jnp.arange(4, dtype=jnp.float32)
    table_angle = -grid_angle[:, None] * wanted[None, :]
    table_cos = jnp.cos(table_angle)
    table_sin = jnp.sin(table_angle)
    highest = lax.Precision.HIGHEST
    numer_real = (
        jnp.dot(sample_real, table_cos, precision=highest)
        - jnp.dot(sample_imag, table_sin, precision=highest)
    ) / NODE_NUMBER
    numer_imag = (
        jnp.dot(sample_real, table_sin, precision=highest)
        + jnp.dot(sample_imag, table_cos, precision=highest)
    ) / NODE_NUMBER
    onehot = (responding_nodes[:, None] == grid_index[None, :]).astype(jnp.float32)
    denom_real = jnp.sum(onehot * sample_real, axis=1)
    denom_imag = jnp.sum(onehot * sample_imag, axis=1)
    magnitude = denom_real * denom_real + denom_imag * denom_imag
    coefficient_actual = (
        numer_real * denom_real[:, None] + numer_imag * denom_imag[:, None]
    ) / magnitude[:, None]
    coefficient_image = (
        numer_imag * denom_real[:, None] - numer_real * denom_imag[:, None]
    ) / magnitude[:, None]
    return (coefficient_actual, coefficient_image)


def encode_kernel(nodes, table, source, out, flags, extra_points, rows, stack):
    for j in range(NODE_NUMBER):
        flags[j] = 0
    for s in range(nodes.shape[0]):
        flags[nodes[s]] = 1
    found = jnp.int32(0)
    for g in range(PAIRS):
        extra_points[found] = 2 * g + 1
        found = found + flags[2 * g] * flags[2 * g + 1]

    rows[...] = source[...].astype(jnp.float32)
    tops = []
    lows = []
    for b in range(8):
        at = 48 * (b // 4) + b % 4
        tops.append(rows[pl.ds(at, 8, stride=4), :])
        low = rows[pl.ds(at + 32, 4, stride=4), :]
        lows.append(jnp.concatenate([low, low], axis=0))
    upper = lax.broadcasted_iota(jnp.int32, (8, 128), 0) < 4

    def block(point):
        at = 16 * point
        real = [table[at + b] for b in range(8)]
        imag = [table[at + 8 + b] for b in range(8)]
        top_r = sum(real[b] * tops[b] for b in range(8))
        top_i = sum(imag[b] * tops[b] for b in range(8))
        low = sum(jnp.where(upper, real[b], imag[b]) * lows[b] for b in range(8))
        return [top_r, top_i, low]

    stack[...] = jnp.zeros_like(stack)
    for e in range(EXTRAS):
        for v, tile in enumerate(block(extra_points[e])):
            stack[24 * e + 8 * v : 24 * e + 8 * v + 8, :] = tile
    stack[...] = stack[...].T

    def main(t, carry):
        parts = block(2 * t + 1 - flags[2 * t])
        parts.append(stack[pl.ds(pl.multiple_of(8 * t, 8), 8), :])
        value = jnp.concatenate(parts, axis=0).astype(jnp.bfloat16)
        out[t] = value
        return carry

    lax.fori_loop(0, PAIRS, main, 0)


def encode(nodes, table, source):
    return pl.pallas_call(
        encode_kernel,
        out_shape=jax.ShapeDtypeStruct((PAIRS, 32, 128), jnp.bfloat16),
        in_specs=[
            pl.BlockSpec(memory_space=pltpu.SMEM),
            pl.BlockSpec(memory_space=pltpu.SMEM),
            pl.BlockSpec(memory_space=pltpu.VMEM),
        ],
        out_specs=pl.BlockSpec(memory_space=pltpu.VMEM),
        scratch_shapes=[
            pltpu.SMEM((NODE_NUMBER,), jnp.int32),
            pltpu.SMEM((PAIRS,), jnp.int32),
            pltpu.VMEM((96, 128), jnp.float32),
            pltpu.VMEM((128, 128), jnp.float32),
        ],
        name="encode",
        interpret=INTERPRET,
    )(nodes, table, source)


def compact_kernel(got, out, rows):
    lane = lax.broadcasted_iota(jnp.int32, (8, 128), 1)
    rows[ROWS + 72 :, :] = jnp.zeros((8, 128), jnp.float32)
    pieces = []
    for g in range(PAIRS):
        block = got[g].astype(jnp.float32)
        rows[24 * g : 24 * g + 24, :] = block[:24]
        pieces.append(block[24:])
    for e in range(EXTRAS):
        for v in range(3):
            tile = jnp.zeros((8, 128), jnp.float32)
            for g in range(PAIRS):
                start = 24 * g - 128 * v
                if start + 24 <= 0 or start >= 128:
                    continue
                moved = pltpu.roll(pieces[g], (start - 24 * e) % 128, 1)
                tile = jnp.where((lane >= start) & (lane < start + 24), moved, tile)
            at = ROWS + 8 * (3 * e + v)
            rows[at : at + 8, :] = tile
    out[...] = rows[...].astype(jnp.bfloat16)


def compact(got):
    return pl.pallas_call(
        compact_kernel,
        out_shape=jax.ShapeDtypeStruct((CHUNK_ROWS, 128), jnp.bfloat16),
        in_specs=[pl.BlockSpec(memory_space=pltpu.VMEM)],
        out_specs=pl.BlockSpec(memory_space=pltpu.VMEM),
        scratch_shapes=[pltpu.VMEM((CHUNK_ROWS, 128), jnp.float32)],
        name="compact",
        interpret=INTERPRET,
    )(got)


def split_pairs(pairs, scratch):
    count = pairs.shape[0] // 2
    scratch[: 2 * count, :] = pairs.astype(jnp.float32)
    real = scratch[pl.ds(0, count, stride=2), :]
    imag = scratch[pl.ds(1, count, stride=2), :]
    return jnp.concatenate([real, imag], axis=1).astype(jnp.bfloat16)


def share_kernel(picks, share, out, scratch):
    for y in range(YS):
        piece = split_pairs(share[0, 256 * y : 256 * y + 256, :], scratch)
        out[0, y % 2, 128 * (y // 2) : 128 * (y // 2) + 128, :] = piece


def split_share(picks, share):
    return pl.pallas_call(
        share_kernel,
        out_shape=jax.ShapeDtypeStruct((XS, 2, 512, 256), jnp.bfloat16),
        grid_spec=pltpu.PrefetchScalarGridSpec(
            num_scalar_prefetch=1,
            grid=(XS,),
            in_specs=[pl.BlockSpec((1, 2048, 128), lambda k, picks: (picks[0], k, 0))],
            out_specs=pl.BlockSpec((1, 2, 512, 256), lambda k, picks: (k, 0, 0, 0)),
            scratch_shapes=[pltpu.VMEM((256, 128), jnp.float32)],
        ),
        name="split_share",
        cost_estimate=pl.CostEstimate(flops=400_000_000, bytes_accessed=4_200_000, transcendentals=0),
        interpret=INTERPRET,
    )(picks, share)


def wide(chunk):
    return jnp.concatenate([chunk[q, :ROWS, :] for q in range(QUADS)], axis=1)


def dot(a, b):
    return jnp.dot(a, b, preferred_element_type=jnp.float32)


EARLY = ((0, True), (0, False), (-1, True), (1, True), (-1, False), (1, False))
LATE = ((2, True), (2, False))


def block_of(picks, kind):
    offset, same = kind
    x = (picks[1] + offset + XS) % XS
    return x, picks[2] if same else 1 - picks[2]


def early_kernel(picks, share, c0, c1, c2, c3, c4, c5, acc):
    for n, (chunk, kind) in enumerate(zip((c0, c1, c2, c3, c4, c5), EARLY)):
        x, parity = block_of(picks, kind)
        term = dot(wide(chunk), share[x, parity])
        if n == 0:
            acc[...] = term
        else:
            acc[...] += term


def early_product(picks, share, chunks):
    return pl.pallas_call(
        early_kernel,
        out_shape=jax.ShapeDtypeStruct((ROWS, 256), jnp.float32),
        in_specs=[pl.BlockSpec(memory_space=pltpu.SMEM)] + [pl.BlockSpec(memory_space=pltpu.VMEM)] * 7,
        out_specs=pl.BlockSpec(memory_space=pltpu.VMEM),
        name="early_product",
        cost_estimate=pl.CostEstimate(flops=400_000_000, bytes_accessed=4_200_000, transcendentals=0),
        interpret=INTERPRET,
    )(picks, share, *chunks)


def late_kernel(
    picks, weights, share, spread, before, c0, c1, c2, c3, c4, c5, c6, c7, out,
    acc, blocks, small, ends, late, extra, acc_extra, scratch, sems,
):
    early = (c0, c1, c2, c3, c4, c5)
    chunks = (c6, c7)
    copies = []

    def start(source, target):
        copy = pltpu.make_async_copy(source, target, sems.at[len(copies)])
        copy.start()
        copies.append(copy)

    start(spread, small)
    for n in range(6):
        start(early[n].at[:, pl.ds(ROWS, 80), :], ends.at[n])
    for n in range(2):
        x, parity = block_of(picks, LATE[n])
        start(chunks[n], late.at[n])
        start(share.at[x, parity], blocks.at[n])
    start(before, acc)

    def place(rows_of, kind):
        x, parity = block_of(picks, kind)
        for q in range(QUADS):
            rows = rows_of(q)
            at = pl.multiple_of(8 * (YS * x + 2 * q + parity), 8)
            for v in range(9):
                extra[pl.ds(at, 8), 128 * v : 128 * v + 128] = rows[8 * v : 8 * v + 8]

    for copy in copies[:7]:
        copy.wait()
    for n in range(6):
        place(lambda q: ends[n, q].astype(jnp.float32), EARLY[n])
    slices = [split_pairs(small[e], scratch) for e in range(EXTRAS)]
    for n in range(2):
        copies[7 + 2 * n].wait()
        place(lambda q: late[n, q, ROWS:, :].astype(jnp.float32), LATE[n])
    for e in range(EXTRAS):
        turned = extra[:, ROWS * e : ROWS * e + ROWS].astype(jnp.bfloat16)
        acc_extra[e] = lax.dot_general(
            turned, slices[e], (((0,), (0,)), ((), ())), preferred_element_type=jnp.float32
        )
    copies[11].wait()
    for n in range(2):
        copies[8 + 2 * n].wait()
        acc[...] += dot(wide(late.at[n]), blocks[n])

    upper = lax.broadcasted_iota(jnp.int32, (8, 128), 0) < 4

    def decode(g, carry):
        top = [jnp.zeros((8, 128), jnp.float32)] * 4
        low = [jnp.zeros((8, 128), jnp.float32)] * 4
        at = pl.multiple_of(24 * g, 8)
        for s in range(1 + EXTRAS):
            tiles = [
                acc[pl.ds(at + 8 * v, 8), :] if s == 0 else acc_extra[s - 1, pl.ds(at + 8 * v, 8), :]
                for v in range(3)
            ]
            top_r = tiles[0][:, :128] - tiles[1][:, 128:]
            top_i = tiles[0][:, 128:] + tiles[1][:, :128]
            low_r = tiles[2][:, :128] - pltpu.roll(tiles[2][:, 128:], 4, 0)
            low_i = tiles[2][:, 128:] + pltpu.roll(tiles[2][:, :128], 4, 0)
            for b in range(4):
                w_r = weights[8 * s + b]
                w_i = weights[8 * s + 4 + b]
                top[b] = top[b] + (w_r * top_r - w_i * top_i)
                low[b] = low[b] + (w_r * low_r - w_i * low_i)
        low_a = jnp.where(upper, low[0], pltpu.roll(low[1], 4, 0))
        low_b = jnp.where(upper, low[2], pltpu.roll(low[3], 4, 0))
        out[g] = jnp.concatenate(top + [low_a, low_b], axis=0)
        return carry

    lax.fori_loop(0, PAIRS, decode, 0)


def late_product(picks, weights, share, spread, before, early, late):
    return pl.pallas_call(
        late_kernel,
        out_shape=jax.ShapeDtypeStruct((PAIRS, 48, 128), jnp.float32),
        in_specs=[pl.BlockSpec(memory_space=pltpu.SMEM)] * 2 + [pl.BlockSpec(memory_space=pl.ANY)] * 11,
        out_specs=pl.BlockSpec(memory_space=pltpu.VMEM),
        scratch_shapes=[
            pltpu.VMEM((ROWS, 256), jnp.float32),
            pltpu.VMEM((2, 512, 256), jnp.bfloat16),
            pltpu.VMEM((EXTRAS, 512, 128), jnp.bfloat16),
            pltpu.VMEM((6, QUADS, 80, 128), jnp.bfloat16),
            pltpu.VMEM((2, QUADS, CHUNK_ROWS, 128), jnp.bfloat16),
            pltpu.VMEM((256, 1152), jnp.float32),
            pltpu.VMEM((EXTRAS, ROWS, 256), jnp.float32),
            pltpu.VMEM((512, 128), jnp.float32),
            pltpu.SemaphoreType.DMA((12,)),
        ],
        name="late_product",
        interpret=INTERPRET,
    )(picks, weights, share, spread, before, *early, *late)


def choose(responding_nodes):
    listed = jnp.any(
        responding_nodes[:, None] == jnp.arange(NODE_NUMBER, dtype=jnp.int32)[None, :], axis=0
    ).reshape(PAIRS, 2)
    both = listed[:, 0] & listed[:, 1]
    index = jnp.arange(PAIRS, dtype=jnp.int32)
    before = jnp.sum((index[None, :] < index[:, None]) & both[None, :], axis=1)
    extra_pair = both[None, :] & (before[None, :] == jnp.arange(EXTRAS, dtype=jnp.int32)[:, None])
    return listed[:, 0], extra_pair


def summed(received):
    total = jnp.sum(received, axis=0)
    top = total[:32].reshape(2, 2, 8, 128)
    low = total[32:].reshape(2, 2, 4, 128)
    return jnp.concatenate([top, low], axis=2).transpose(0, 2, 1, 3)


def decode_weights(nodes, group, second):
    coefficient_actual, coefficient_image = recovery_coefficients(nodes)
    _, extra_pair = choose(nodes)
    extra_group = jnp.sum(
        jnp.where(extra_pair, jnp.arange(PAIRS, dtype=jnp.int32)[None, :], 0), axis=1
    ).astype(jnp.int32)
    used = jnp.concatenate([(2 * group + second)[None], 2 * extra_group + 1])
    point_selector = (used[:, None] == nodes[None, :])[:, :, None]
    weights = jnp.concatenate(
        [
            jnp.sum(jnp.where(point_selector, coefficient_actual[None], 0.0), axis=1),
            jnp.sum(jnp.where(point_selector, coefficient_image[None], 0.0), axis=1),
        ],
        axis=1,
    ).reshape(-1)
    return weights, extra_group


def shards(source_matrix_tiles, second_operand_encoded, responding_nodes):
    sent = encode(
        responding_nodes, jnp.asarray(trig_table().reshape(-1)), source_matrix_tiles.reshape(96, 128)
    )
    got = lax.all_to_all(sent, "group", split_axis=0, concat_axis=0, tiled=True)

    odd = second_operand_encoded[1].reshape(PANELS, PAIRS, 8, 2, 128).transpose(1, 0, 2, 3, 4)
    odd, got = lax.optimization_barrier((odd, got))
    spread = lax.all_to_all(odd, "group", split_axis=0, concat_axis=0, tiled=True)
    even_listed, _ = choose(responding_nodes)
    group = lax.axis_index("group")
    second = jnp.where(even_listed[group], 0, 1).astype(jnp.int32)
    picks = jnp.stack([second, lax.axis_index("x"), lax.axis_index("parity")]).astype(jnp.int32)
    a = lax.all_gather(compact(got), "quad")

    def hop(chunk, axis, size, by):
        return lax.ppermute(chunk, axis, [(i, (i + by) % size) for i in range(size)])

    y_axes = ("quad", "parity")
    nodes, whole, a = lax.optimization_barrier((responding_nodes, second_operand_encoded, a))
    right_a = hop(a, "x", XS, 1)
    left_a = hop(a, "x", XS, -1)
    b = hop(a, y_axes, YS, -1)
    right_b = hop(right_a, y_axes, YS, 1)
    left_b = hop(left_a, y_axes, YS, -1)
    far_a = hop(right_a, "x", XS, 1)
    far_b = hop(left_b, "x", XS, -1)
    share = split_share(picks, whole.reshape(2, 8192, 128))

    weights, extra_group = decode_weights(nodes, group, second)
    early = (a, b, right_a, left_a, right_b, left_b)
    before = early_product(picks, share, early)
    three = jnp.stack(
        [lax.dynamic_index_in_dim(spread, extra_group[e], 0, keepdims=False) for e in range(EXTRAS)]
    ).reshape(EXTRAS, 512, 128)
    partial = late_product(picks, weights, share, three, before, early, (far_a, far_b))
    received = lax.all_to_all(partial, "group", split_axis=0, concat_axis=0, tiled=True)
    return summed(received)


def solution(mesh):
    torus = Mesh(
        mesh.devices.reshape(mesh.shape["group"], XS, QUADS, 2), ("group", "x", "quad", "parity")
    )
    panel = ("x", "quad", "parity")
    return jax.shard_map(
        shards,
        mesh=torus,
        in_specs=(P(None, "group", None, panel), P("group", None, None, panel), P()),
        out_specs=P(None, "group", None, panel),
        check_vma=False,
    )
```

```python
import math

import jax
import jax.numpy as jnp
import numpy as np
from jax import lax
from jax.experimental import pallas as pl
from jax.experimental.pallas import tpu as pltpu
from jax.sharding import Mesh
from jax.sharding import PartitionSpec as P


NODE_NUMBER = 32
PAIRS = 16
EXTRAS = 3
XS = 4
YS = 8
QUADS = YS // 2
PANELS = XS * YS
ROWS = 384
CHUNK_ROWS = 464
INTERPRET = False

TWO_PI_RADIANS = 2.0 * math.pi


def trig_table():
    exponent = np.arange(4, dtype=np.float32)[None, :] + 8 * np.arange(2, dtype=np.float32)[:, None]
    point = np.arange(NODE_NUMBER, dtype=np.float32)
    phase = np.float32(TWO_PI_RADIANS) * point / np.float32(NODE_NUMBER)
    angle = (phase[:, None, None] * exponent[None]).astype(np.float64)
    table = np.stack([np.cos(angle), np.sin(angle)], axis=1)
    return table.reshape(NODE_NUMBER, 16).astype(np.float32)


def grid_table():
    grid = np.float32(TWO_PI_RADIANS) * np.arange(NODE_NUMBER, dtype=np.float32) / np.float32(NODE_NUMBER)
    wanted = (3 + 4 * np.arange(4)).astype(np.float32)
    turns = (-grid[None, :] * wanted[:, None]).astype(np.float64)
    grid = grid.astype(np.float64)
    rows = np.zeros((16, 128), np.float32)
    rows[0, :NODE_NUMBER] = np.cos(grid)
    rows[1, :NODE_NUMBER] = np.sin(grid)
    rows[2:6, :NODE_NUMBER] = np.cos(turns)
    rows[6:10, :NODE_NUMBER] = np.sin(turns)
    return rows


def weights_kernel(nodes, picks, points, grid, out):
    number = nodes.shape[0]
    shape = (24, 128)
    row = lax.broadcasted_iota(jnp.int32, shape, 0)
    lane = lax.broadcasted_iota(jnp.int32, shape, 1)
    real = jnp.ones(shape, jnp.float32)
    imag = jnp.zeros(shape, jnp.float32)
    node = jnp.full(shape, -1, jnp.int32)
    for t in range(number):
        mine = row == t
        node = jnp.where(mine, nodes[t], node)
        step_r = jnp.where(mine, 1.0, grid[0:1, :] - points[nodes[t]])
        step_i = jnp.where(mine, 0.0, grid[1:2, :] - points[NODE_NUMBER + nodes[t]])
        real, imag = real * step_r - imag * step_i, real * step_i + imag * step_r

    def across(value):
        return jnp.sum(value, axis=1, keepdims=True)

    here = node == lane
    denom_r = across(jnp.where(here, real, 0.0))
    denom_i = across(jnp.where(here, imag, 0.0))
    magnitude = denom_r * denom_r + denom_i * denom_i
    for e in range(4):
        cos, sin = grid[2 + e : 3 + e, :], grid[6 + e : 7 + e, :]
        numer_r = across(real * cos - imag * sin) / NODE_NUMBER
        numer_i = across(real * sin + imag * cos) / NODE_NUMBER
        weight_r = (numer_r * denom_r + numer_i * denom_i) / magnitude
        weight_i = (numer_i * denom_r - numer_r * denom_i) / magnitude
        for c in range(1 + EXTRAS):
            chosen = node == picks[8 + c]
            out[8 * c + e : 8 * c + e + 1, :] = jnp.sum(
                jnp.where(chosen, weight_r, 0.0), axis=0, keepdims=True
            )
            out[8 * c + 4 + e : 8 * c + 5 + e, :] = jnp.sum(
                jnp.where(chosen, weight_i, 0.0), axis=0, keepdims=True
            )


def decode_weights(nodes, picks):
    grid = grid_table()
    points = grid[:2, :NODE_NUMBER].reshape(-1)
    return pl.pallas_call(
        weights_kernel,
        out_shape=jax.ShapeDtypeStruct((32, 128), jnp.float32),
        in_specs=[pl.BlockSpec(memory_space=pltpu.SMEM)] * 3 + [pl.BlockSpec(memory_space=pltpu.VMEM)],
        out_specs=pl.BlockSpec(memory_space=pltpu.VMEM),
        name="weights",
        interpret=INTERPRET,
    )(nodes, picks, jnp.asarray(points), jnp.asarray(grid))


def encode_kernel(place, nodes, table, source, out, picks, flags, extra_points, rows, stack):
    for j in range(NODE_NUMBER):
        flags[j] = 0
    for s in range(nodes.shape[0]):
        flags[nodes[s]] = 1
    found = jnp.int32(0)
    for g in range(PAIRS):
        extra_points[found] = 2 * g + 1
        found = found + flags[2 * g] * flags[2 * g + 1]
    second = 1 - flags[2 * place[0]]
    picks[0] = second
    picks[1] = place[1]
    picks[2] = place[2]
    picks[3] = place[0] % 2
    picks[8] = 2 * place[0] + second
    for e in range(EXTRAS):
        picks[4 + e] = (extra_points[e] - 1) // 2
        picks[9 + e] = extra_points[e]

    rows[...] = source[...].astype(jnp.float32)
    tops = []
    lows = []
    for b in range(8):
        at = 48 * (b // 4) + b % 4
        tops.append(rows[pl.ds(at, 8, stride=4), :])
        low = rows[pl.ds(at + 32, 4, stride=4), :]
        lows.append(jnp.concatenate([low, low], axis=0))
    upper = lax.broadcasted_iota(jnp.int32, (8, 128), 0) < 4

    def block(point):
        at = 16 * point
        real = [table[at + b] for b in range(8)]
        imag = [table[at + 8 + b] for b in range(8)]
        top_r = sum(real[b] * tops[b] for b in range(8))
        top_i = sum(imag[b] * tops[b] for b in range(8))
        low = sum(jnp.where(upper, real[b], imag[b]) * lows[b] for b in range(8))
        return [top_r, top_i, low]

    stack[...] = jnp.zeros_like(stack)
    for e in range(EXTRAS):
        for v, tile in enumerate(block(extra_points[e])):
            stack[24 * e + 8 * v : 24 * e + 8 * v + 8, :] = tile
    stack[...] = stack[...].T

    def main(t, carry):
        parts = block(2 * t + 1 - flags[2 * t])
        parts.append(stack[pl.ds(pl.multiple_of(8 * t, 8), 8), :])
        value = jnp.concatenate(parts, axis=0).astype(jnp.bfloat16)
        out[t] = value
        return carry

    lax.fori_loop(0, PAIRS, main, 0)


def encode(place, nodes, table, source):
    return pl.pallas_call(
        encode_kernel,
        out_shape=(
            jax.ShapeDtypeStruct((PAIRS, 32, 128), jnp.bfloat16),
            jax.ShapeDtypeStruct((16,), jnp.int32),
        ),
        in_specs=[pl.BlockSpec(memory_space=pltpu.SMEM)] * 3 + [pl.BlockSpec(memory_space=pltpu.VMEM)],
        out_specs=(pl.BlockSpec(memory_space=pltpu.VMEM), pl.BlockSpec(memory_space=pltpu.SMEM)),
        scratch_shapes=[
            pltpu.SMEM((NODE_NUMBER,), jnp.int32),
            pltpu.SMEM((PAIRS,), jnp.int32),
            pltpu.VMEM((96, 128), jnp.float32),
            pltpu.VMEM((128, 128), jnp.float32),
        ],
        name="encode",
        interpret=INTERPRET,
    )(place, nodes, table, source)


def compact_kernel(got, out, rows):
    lane = lax.broadcasted_iota(jnp.int32, (8, 128), 1)
    rows[ROWS + 72 :, :] = jnp.zeros((8, 128), jnp.float32)
    pieces = []
    for g in range(PAIRS):
        block = got[g].astype(jnp.float32)
        rows[24 * g : 24 * g + 24, :] = block[:24]
        pieces.append(block[24:])
    for e in range(EXTRAS):
        for v in range(3):
            tile = jnp.zeros((8, 128), jnp.float32)
            for g in range(PAIRS):
                start = 24 * g - 128 * v
                if start + 24 <= 0 or start >= 128:
                    continue
                moved = pltpu.roll(pieces[g], (start - 24 * e) % 128, 1)
                tile = jnp.where((lane >= start) & (lane < start + 24), moved, tile)
            at = ROWS + 8 * (3 * e + v)
            rows[at : at + 8, :] = tile
    out[...] = rows[...].astype(jnp.bfloat16)


def compact(got):
    return pl.pallas_call(
        compact_kernel,
        out_shape=jax.ShapeDtypeStruct((CHUNK_ROWS, 128), jnp.bfloat16),
        in_specs=[pl.BlockSpec(memory_space=pltpu.VMEM)],
        out_specs=pl.BlockSpec(memory_space=pltpu.VMEM),
        scratch_shapes=[pltpu.VMEM((CHUNK_ROWS, 128), jnp.float32)],
        name="compact",
        interpret=INTERPRET,
    )(got)


def split_pairs(pairs, scratch):
    count = pairs.shape[0] // 2
    scratch[: 2 * count, :] = pairs.astype(jnp.float32)
    real = scratch[pl.ds(0, count, stride=2), :]
    imag = scratch[pl.ds(1, count, stride=2), :]
    return jnp.concatenate([real, imag], axis=1).astype(jnp.bfloat16)


def share_kernel(picks, share, out, scratch):
    for y in range(YS):
        piece = split_pairs(share[0, 256 * y : 256 * y + 256, :], scratch)
        out[0, y % 2, 128 * (y // 2) : 128 * (y // 2) + 128, :] = piece


def split_share(picks, share):
    return pl.pallas_call(
        share_kernel,
        out_shape=jax.ShapeDtypeStruct((XS, 2, 512, 256), jnp.bfloat16),
        grid_spec=pltpu.PrefetchScalarGridSpec(
            num_scalar_prefetch=1,
            grid=(XS,),
            in_specs=[pl.BlockSpec((1, 2048, 128), lambda k, picks: (picks[0], k, 0))],
            out_specs=pl.BlockSpec((1, 2, 512, 256), lambda k, picks: (k, 0, 0, 0)),
            scratch_shapes=[pltpu.VMEM((256, 128), jnp.float32)],
        ),
        name="split_share",
        cost_estimate=pl.CostEstimate(flops=400_000_000, bytes_accessed=4_200_000, transcendentals=0),
        interpret=INTERPRET,
    )(picks, share)


def wide(chunk):
    return jnp.concatenate([chunk[q, :ROWS, :] for q in range(QUADS)], axis=1)


def dot(a, b):
    return jnp.dot(a, b, preferred_element_type=jnp.float32)


EARLY = ((0, True), (0, False), (-1, True), (1, True), (-1, False), (1, False))
LATE = ((2, True), (2, False))


def block_of(picks, kind):
    offset, same = kind
    x = (picks[1] + offset + XS) % XS
    return x, picks[2] if same else 1 - picks[2]


def early_kernel(picks, share, c0, c1, c2, c3, c4, c5, acc):
    for n, (chunk, kind) in enumerate(zip((c0, c1, c2, c3, c4, c5), EARLY)):
        x, parity = block_of(picks, kind)
        term = dot(wide(chunk), share[x, parity])
        if n == 0:
            acc[...] = term
        else:
            acc[...] += term


def early_product(picks, share, chunks):
    return pl.pallas_call(
        early_kernel,
        out_shape=jax.ShapeDtypeStruct((ROWS, 256), jnp.float32),
        in_specs=[pl.BlockSpec(memory_space=pltpu.SMEM)] + [pl.BlockSpec(memory_space=pltpu.VMEM)] * 7,
        out_specs=pl.BlockSpec(memory_space=pltpu.VMEM),
        name="early_product",
        cost_estimate=pl.CostEstimate(flops=400_000_000, bytes_accessed=4_200_000, transcendentals=0),
        interpret=INTERPRET,
    )(picks, share, *chunks)


def late_kernel(
    picks, weights, share, s0, s1, s2, before, c0, c1, c2, c3, c4, c5, c6, c7, kept, sent,
    acc, blocks, small, ends, late, extra, acc_extra, scratch, sems,
):
    early = (c0, c1, c2, c3, c4, c5)
    chunks = (c6, c7)
    copies = []

    def start(source, target):
        copy = pltpu.make_async_copy(source, target, sems.at[len(copies)])
        copy.start()
        copies.append(copy)

    for e, part in enumerate((s0, s1, s2)):
        start(part, small.at[e])
    for n in range(6):
        start(early[n].at[:, pl.ds(ROWS, 80), :], ends.at[n])
    for n in range(2):
        x, parity = block_of(picks, LATE[n])
        start(chunks[n], late.at[n])
        start(share.at[x, parity], blocks.at[n])
    start(before, acc)

    def place(rows_of, kind):
        x, parity = block_of(picks, kind)
        for q in range(QUADS):
            rows = rows_of(q)
            at = pl.multiple_of(8 * (YS * x + 2 * q + parity), 8)
            for v in range(9):
                extra[pl.ds(at, 8), 128 * v : 128 * v + 128] = rows[8 * v : 8 * v + 8]

    for copy in copies[:9]:
        copy.wait()
    for n in range(6):
        place(lambda q: ends[n, q].astype(jnp.float32), EARLY[n])
    slices = [split_pairs(small[e], scratch) for e in range(EXTRAS)]
    for n in range(2):
        copies[9 + 2 * n].wait()
        place(lambda q: late[n, q, ROWS:, :].astype(jnp.float32), LATE[n])
    for e in range(EXTRAS):
        turned = extra[:, ROWS * e : ROWS * e + ROWS].astype(jnp.bfloat16)
        acc_extra[e] = lax.dot_general(
            turned, slices[e], (((0,), (0,)), ((), ())), preferred_element_type=jnp.float32
        )
    copies[13].wait()
    for n in range(2):
        copies[10 + 2 * n].wait()
        acc[...] += dot(wide(late.at[n]), blocks[n])

    upper = lax.broadcasted_iota(jnp.int32, (8, 128), 0) < 4

    def decode(g):
        top = [jnp.zeros((8, 128), jnp.float32)] * 4
        low = [jnp.zeros((8, 128), jnp.float32)] * 4
        at = pl.multiple_of(24 * g, 8)
        for s in range(1 + EXTRAS):
            tiles = [
                acc[pl.ds(at + 8 * v, 8), :] if s == 0 else acc_extra[s - 1, pl.ds(at + 8 * v, 8), :]
                for v in range(3)
            ]
            top_r = tiles[0][:, :128] - tiles[1][:, 128:]
            top_i = tiles[0][:, 128:] + tiles[1][:, :128]
            low_r = tiles[2][:, :128] - pltpu.roll(tiles[2][:, 128:], 4, 0)
            low_i = tiles[2][:, 128:] + pltpu.roll(tiles[2][:, :128], 4, 0)
            for b in range(4):
                w_r = weights[8 * s + b : 8 * s + b + 1, :]
                w_i = weights[8 * s + 4 + b : 8 * s + 5 + b, :]
                top[b] = top[b] + (w_r * top_r - w_i * top_i)
                low[b] = low[b] + (w_r * low_r - w_i * low_i)
        low_a = jnp.where(upper, low[0], pltpu.roll(low[1], 4, 0))
        low_b = jnp.where(upper, low[2], pltpu.roll(low[3], 4, 0))
        return jnp.concatenate(top + [low_a, low_b], axis=0)

    core = picks[3]

    def both(z, carry):
        kept[z] = decode(2 * z + core)
        sent[z] = decode(2 * z + 1 - core)
        return carry

    lax.fori_loop(0, PAIRS // 2, both, 0)


def late_product(picks, weights, share, spread, before, early, late):
    return pl.pallas_call(
        late_kernel,
        out_shape=(jax.ShapeDtypeStruct((PAIRS // 2, 48, 128), jnp.float32),) * 2,
        in_specs=[pl.BlockSpec(memory_space=pltpu.SMEM), pl.BlockSpec(memory_space=pltpu.VMEM)]
        + [pl.BlockSpec(memory_space=pl.ANY)] * 13,
        out_specs=(pl.BlockSpec(memory_space=pltpu.VMEM),) * 2,
        scratch_shapes=[
            pltpu.VMEM((ROWS, 256), jnp.float32),
            pltpu.VMEM((2, 512, 256), jnp.bfloat16),
            pltpu.VMEM((EXTRAS, 512, 128), jnp.bfloat16),
            pltpu.VMEM((6, QUADS, 80, 128), jnp.bfloat16),
            pltpu.VMEM((2, QUADS, CHUNK_ROWS, 128), jnp.bfloat16),
            pltpu.VMEM((256, 1152), jnp.float32),
            pltpu.VMEM((EXTRAS, ROWS, 256), jnp.float32),
            pltpu.VMEM((512, 128), jnp.float32),
            pltpu.SemaphoreType.DMA((14,)),
        ],
        name="late_product",
        interpret=INTERPRET,
    )(picks, weights, share, *spread, before, *early, *late)


def summed(received):
    total = jnp.sum(received, axis=0)
    top = total[:32].reshape(2, 2, 8, 128)
    low = total[32:].reshape(2, 2, 4, 128)
    return jnp.concatenate([top, low], axis=2).transpose(0, 2, 1, 3)


def shards(source_matrix_tiles, second_operand_encoded, responding_nodes):
    group = ("z", "core")
    place = jnp.stack([lax.axis_index(group), lax.axis_index("x"), lax.axis_index("parity")])
    sent, picks = encode(
        place.astype(jnp.int32),
        responding_nodes,
        jnp.asarray(trig_table().reshape(-1)),
        source_matrix_tiles.reshape(96, 128),
    )
    got = lax.all_to_all(sent, group, split_axis=0, concat_axis=0, tiled=True)

    odd = second_operand_encoded[1].reshape(PANELS, PAIRS, 8, 2, 128).transpose(1, 0, 2, 3, 4)
    odd, got = lax.optimization_barrier((odd, got))
    spread = lax.all_to_all(odd, group, split_axis=0, concat_axis=0, tiled=True)
    a = lax.all_gather(compact(got), "quad")

    def hop(chunk, axis, size, by):
        return lax.ppermute(chunk, axis, [(i, (i + by) % size) for i in range(size)])

    y_axes = ("quad", "parity")
    nodes, whole, a = lax.optimization_barrier((responding_nodes, second_operand_encoded, a))
    right_a = hop(a, "x", XS, 1)
    left_a = hop(a, "x", XS, -1)
    b = hop(a, y_axes, YS, -1)
    right_b = hop(right_a, y_axes, YS, 1)
    left_b = hop(left_a, y_axes, YS, -1)
    far_a = hop(right_a, "x", XS, 1)
    far_b = hop(left_b, "x", XS, -1)
    share = split_share(picks, whole.reshape(2, 8192, 128))
    weights = decode_weights(nodes, picks)
    early = (a, b, right_a, left_a, right_b, left_b)
    before = early_product(picks, share, early)
    three = [
        lax.dynamic_index_in_dim(spread, picks[4 + e], 0, keepdims=False).reshape(512, 128)
        for e in range(EXTRAS)
    ]
    kept, passed = late_product(picks, weights, share, three, before, early, (far_a, far_b))
    kept = kept + lax.ppermute(passed, "core", [(0, 1), (1, 0)])
    received = lax.all_to_all(kept, "z", split_axis=0, concat_axis=0, tiled=True)
    return summed(received)


def solution(mesh):
    torus = Mesh(
        mesh.devices.reshape(PAIRS // 2, 2, XS, QUADS, 2), ("z", "core", "x", "quad", "parity")
    )
    group = ("z", "core")
    panel = ("x", "quad", "parity")
    return jax.shard_map(
        shards,
        mesh=torus,
        in_specs=(P(None, group, None, panel), P(group, None, None, panel), P()),
        out_specs=P(None, group, None, panel),
        check_vma=False,
    )
```

```python
import math

import jax
import jax.numpy as jnp
import numpy as np
from jax import lax
from jax.experimental import pallas as pl
from jax.experimental.pallas import tpu as pltpu
from jax.sharding import Mesh
from jax.sharding import PartitionSpec as P


NODE_NUMBER = 32
PAIRS = 16
EXTRAS = 3
XS = 4
YS = 8
QUADS = YS // 2
PANELS = XS * YS
ROWS = 384
CHUNK_ROWS = 464
INTERPRET = False

TWO_PI_RADIANS = 2.0 * math.pi


def trig_table():
    exponent = np.arange(4, dtype=np.float32)[None, :] + 8 * np.arange(2, dtype=np.float32)[:, None]
    point = np.arange(NODE_NUMBER, dtype=np.float32)
    phase = np.float32(TWO_PI_RADIANS) * point / np.float32(NODE_NUMBER)
    angle = (phase[:, None, None] * exponent[None]).astype(np.float64)
    table = np.stack([np.cos(angle), np.sin(angle)], axis=1)
    return table.reshape(NODE_NUMBER, 16).astype(np.float32)


def grid_table():
    grid = np.float32(TWO_PI_RADIANS) * np.arange(NODE_NUMBER, dtype=np.float32) / np.float32(NODE_NUMBER)
    wanted = (3 + 4 * np.arange(4)).astype(np.float32)
    turns = (-grid[None, :] * wanted[:, None]).astype(np.float64)
    grid = grid.astype(np.float64)
    rows = np.zeros((16, 128), np.float32)
    rows[0, :NODE_NUMBER] = np.cos(grid)
    rows[1, :NODE_NUMBER] = np.sin(grid)
    rows[2:6, :NODE_NUMBER] = np.cos(turns)
    rows[6:10, :NODE_NUMBER] = np.sin(turns)
    return rows


def weights_kernel(nodes, picks, points, grid, out):
    number = nodes.shape[0]
    shape = (24, 128)
    row = lax.broadcasted_iota(jnp.int32, shape, 0)
    lane = lax.broadcasted_iota(jnp.int32, shape, 1)
    real = jnp.ones(shape, jnp.float32)
    imag = jnp.zeros(shape, jnp.float32)
    node = jnp.full(shape, -1, jnp.int32)
    for t in range(number):
        mine = row == t
        node = jnp.where(mine, nodes[t], node)
        step_r = jnp.where(mine, 1.0, grid[0:1, :] - points[nodes[t]])
        step_i = jnp.where(mine, 0.0, grid[1:2, :] - points[NODE_NUMBER + nodes[t]])
        real, imag = real * step_r - imag * step_i, real * step_i + imag * step_r

    def across(value):
        return jnp.sum(value, axis=1, keepdims=True)

    here = node == lane
    denom_r = across(jnp.where(here, real, 0.0))
    denom_i = across(jnp.where(here, imag, 0.0))
    magnitude = denom_r * denom_r + denom_i * denom_i
    for e in range(4):
        cos, sin = grid[2 + e : 3 + e, :], grid[6 + e : 7 + e, :]
        numer_r = across(real * cos - imag * sin) / NODE_NUMBER
        numer_i = across(real * sin + imag * cos) / NODE_NUMBER
        weight_r = (numer_r * denom_r + numer_i * denom_i) / magnitude
        weight_i = (numer_i * denom_r - numer_r * denom_i) / magnitude
        for c in range(1 + EXTRAS):
            chosen = node == picks[8 + c]
            out[8 * c + e : 8 * c + e + 1, :] = jnp.sum(
                jnp.where(chosen, weight_r, 0.0), axis=0, keepdims=True
            )
            out[8 * c + 4 + e : 8 * c + 5 + e, :] = jnp.sum(
                jnp.where(chosen, weight_i, 0.0), axis=0, keepdims=True
            )


def decode_weights(nodes, picks):
    grid = grid_table()
    points = grid[:2, :NODE_NUMBER].reshape(-1)
    return pl.pallas_call(
        weights_kernel,
        out_shape=jax.ShapeDtypeStruct((32, 128), jnp.float32),
        in_specs=[pl.BlockSpec(memory_space=pltpu.SMEM)] * 3 + [pl.BlockSpec(memory_space=pltpu.VMEM)],
        out_specs=pl.BlockSpec(memory_space=pltpu.VMEM),
        name="weights",
        interpret=INTERPRET,
    )(nodes, picks, jnp.asarray(points), jnp.asarray(grid))


def position():
    group = 2 * lax.axis_index("z") + lax.axis_index("core")
    return group, lax.axis_index("x"), lax.axis_index("parity")


def encode_kernel(nodes, table, source, out, picks, flags, extra_points, rows, stack):
    for j in range(NODE_NUMBER):
        flags[j] = 0
    for s in range(nodes.shape[0]):
        flags[nodes[s]] = 1
    found = jnp.int32(0)
    for g in range(PAIRS):
        extra_points[found] = 2 * g + 1
        found = found + flags[2 * g] * flags[2 * g + 1]
    group, x, parity = position()
    second = 1 - flags[2 * group]
    picks[0] = second
    picks[1] = x
    picks[2] = parity
    picks[3] = group % 2
    picks[8] = 2 * group + second
    for e in range(EXTRAS):
        picks[4 + e] = (extra_points[e] - 1) // 2
        picks[9 + e] = extra_points[e]

    rows[...] = source[...].astype(jnp.float32)
    tops = []
    lows = []
    for b in range(8):
        at = 48 * (b // 4) + b % 4
        tops.append(rows[pl.ds(at, 8, stride=4), :])
        low = rows[pl.ds(at + 32, 4, stride=4), :]
        lows.append(jnp.concatenate([low, low], axis=0))
    upper = lax.broadcasted_iota(jnp.int32, (8, 128), 0) < 4

    def block(point):
        at = 16 * point
        real = [table[at + b] for b in range(8)]
        imag = [table[at + 8 + b] for b in range(8)]
        top_r = sum(real[b] * tops[b] for b in range(8))
        top_i = sum(imag[b] * tops[b] for b in range(8))
        low = sum(jnp.where(upper, real[b], imag[b]) * lows[b] for b in range(8))
        return [top_r, top_i, low]

    stack[...] = jnp.zeros_like(stack)
    for e in range(EXTRAS):
        for v, tile in enumerate(block(extra_points[e])):
            stack[24 * e + 8 * v : 24 * e + 8 * v + 8, :] = tile
    stack[...] = stack[...].T

    def main(t, carry):
        parts = block(2 * t + 1 - flags[2 * t])
        parts.append(stack[pl.ds(pl.multiple_of(8 * t, 8), 8), :])
        value = jnp.concatenate(parts, axis=0).astype(jnp.bfloat16)
        out[t] = value
        return carry

    lax.fori_loop(0, PAIRS, main, 0)


def encode(nodes, table, source):
    return pl.pallas_call(
        encode_kernel,
        out_shape=(
            jax.ShapeDtypeStruct((PAIRS, 32, 128), jnp.bfloat16),
            jax.ShapeDtypeStruct((16,), jnp.int32),
        ),
        in_specs=[pl.BlockSpec(memory_space=pltpu.SMEM)] * 2 + [pl.BlockSpec(memory_space=pltpu.VMEM)],
        out_specs=(pl.BlockSpec(memory_space=pltpu.VMEM), pl.BlockSpec(memory_space=pltpu.SMEM)),
        scratch_shapes=[
            pltpu.SMEM((NODE_NUMBER,), jnp.int32),
            pltpu.SMEM((PAIRS,), jnp.int32),
            pltpu.VMEM((96, 128), jnp.float32),
            pltpu.VMEM((128, 128), jnp.float32),
        ],
        name="encode",
        interpret=INTERPRET,
    )(nodes, table, source)


def compact_kernel(got, out, rows):
    lane = lax.broadcasted_iota(jnp.int32, (8, 128), 1)
    rows[ROWS + 72 :, :] = jnp.zeros((8, 128), jnp.float32)
    pieces = []
    for g in range(PAIRS):
        block = got[g].astype(jnp.float32)
        rows[24 * g : 24 * g + 24, :] = block[:24]
        pieces.append(block[24:])
    for e in range(EXTRAS):
        for v in range(3):
            tile = jnp.zeros((8, 128), jnp.float32)
            for g in range(PAIRS):
                start = 24 * g - 128 * v
                if start + 24 <= 0 or start >= 128:
                    continue
                moved = pltpu.roll(pieces[g], (start - 24 * e) % 128, 1)
                tile = jnp.where((lane >= start) & (lane < start + 24), moved, tile)
            at = ROWS + 8 * (3 * e + v)
            rows[at : at + 8, :] = tile
    out[...] = rows[...].astype(jnp.bfloat16)


def compact(got):
    return pl.pallas_call(
        compact_kernel,
        out_shape=jax.ShapeDtypeStruct((CHUNK_ROWS, 128), jnp.bfloat16),
        in_specs=[pl.BlockSpec(memory_space=pltpu.VMEM)],
        out_specs=pl.BlockSpec(memory_space=pltpu.VMEM),
        scratch_shapes=[pltpu.VMEM((CHUNK_ROWS, 128), jnp.float32)],
        name="compact",
        interpret=INTERPRET,
    )(got)


def split_pairs(pairs, scratch):
    count = pairs.shape[0] // 2
    scratch[: 2 * count, :] = pairs.astype(jnp.float32)
    real = scratch[pl.ds(0, count, stride=2), :]
    imag = scratch[pl.ds(1, count, stride=2), :]
    return jnp.concatenate([real, imag], axis=1).astype(jnp.bfloat16)


def share_kernel(picks, share, out, scratch):
    for y in range(YS):
        piece = split_pairs(share[0, 256 * y : 256 * y + 256, :], scratch)
        out[0, y % 2, 128 * (y // 2) : 128 * (y // 2) + 128, :] = piece


def split_share(picks, share):
    return pl.pallas_call(
        share_kernel,
        out_shape=jax.ShapeDtypeStruct((XS, 2, 512, 256), jnp.bfloat16),
        grid_spec=pltpu.PrefetchScalarGridSpec(
            num_scalar_prefetch=1,
            grid=(XS,),
            in_specs=[pl.BlockSpec((1, 2048, 128), lambda k, picks: (picks[0], k, 0))],
            out_specs=pl.BlockSpec((1, 2, 512, 256), lambda k, picks: (k, 0, 0, 0)),
            scratch_shapes=[pltpu.VMEM((256, 128), jnp.float32)],
        ),
        name="split_share",
        cost_estimate=pl.CostEstimate(flops=400_000_000, bytes_accessed=4_200_000, transcendentals=0),
        interpret=INTERPRET,
    )(picks, share)


def wide(chunk):
    return jnp.concatenate([chunk[q, :ROWS, :] for q in range(QUADS)], axis=1)


def dot(a, b):
    return jnp.dot(a, b, preferred_element_type=jnp.float32)


EARLY = ((0, True), (0, False), (-1, True), (1, True), (-1, False), (1, False))
LATE = ((2, True), (2, False))


def block_of(picks, kind):
    offset, same = kind
    x = (picks[1] + offset + XS) % XS
    return x, picks[2] if same else 1 - picks[2]


def early_kernel(picks, share, c0, c1, c2, c3, c4, c5, acc):
    for n, (chunk, kind) in enumerate(zip((c0, c1, c2, c3, c4, c5), EARLY)):
        x, parity = block_of(picks, kind)
        term = dot(wide(chunk), share[x, parity])
        if n == 0:
            acc[...] = term
        else:
            acc[...] += term


def early_product(picks, share, chunks):
    return pl.pallas_call(
        early_kernel,
        out_shape=jax.ShapeDtypeStruct((ROWS, 256), jnp.float32),
        in_specs=[pl.BlockSpec(memory_space=pltpu.SMEM)] + [pl.BlockSpec(memory_space=pltpu.VMEM)] * 7,
        out_specs=pl.BlockSpec(memory_space=pltpu.VMEM),
        name="early_product",
        cost_estimate=pl.CostEstimate(flops=400_000_000, bytes_accessed=4_200_000, transcendentals=0),
        interpret=INTERPRET,
    )(picks, share, *chunks)


def late_kernel(
    picks, weights, share, spread, before, c0, c1, c2, c3, c4, c5, c6, c7, kept, sent,
    acc, blocks, small, ends, late, extra, acc_extra, scratch, sems,
):
    early = (c0, c1, c2, c3, c4, c5)
    chunks = (c6, c7)
    copies = []

    def start(source, target):
        copy = pltpu.make_async_copy(source, target, sems.at[len(copies)])
        copy.start()
        copies.append(copy)

    for e in range(EXTRAS):
        start(spread.at[picks[4 + e]], small.at[e])
    for n in range(6):
        start(early[n].at[:, pl.ds(ROWS, 80), :], ends.at[n])
    for n in range(2):
        x, parity = block_of(picks, LATE[n])
        start(chunks[n], late.at[n])
        start(share.at[x, parity], blocks.at[n])
    start(before, acc)

    def place(rows_of, kind):
        x, parity = block_of(picks, kind)
        for q in range(QUADS):
            rows = rows_of(q)
            at = pl.multiple_of(8 * (YS * x + 2 * q + parity), 8)
            for v in range(9):
                extra[pl.ds(at, 8), 128 * v : 128 * v + 128] = rows[8 * v : 8 * v + 8]

    for copy in copies[:9]:
        copy.wait()
    for n in range(6):
        place(lambda q: ends[n, q].astype(jnp.float32), EARLY[n])
    slices = [split_pairs(small[e], scratch) for e in range(EXTRAS)]
    for n in range(2):
        copies[9 + 2 * n].wait()
        place(lambda q: late[n, q, ROWS:, :].astype(jnp.float32), LATE[n])
    for e in range(EXTRAS):
        turned = extra[:, ROWS * e : ROWS * e + ROWS].astype(jnp.bfloat16)
        acc_extra[e] = lax.dot_general(
            turned, slices[e], (((0,), (0,)), ((), ())), preferred_element_type=jnp.float32
        )
    copies[13].wait()
    for n in range(2):
        copies[10 + 2 * n].wait()
        acc[...] += dot(wide(late.at[n]), blocks[n])

    upper = lax.broadcasted_iota(jnp.int32, (8, 128), 0) < 4

    def decode(g):
        top = [jnp.zeros((8, 128), jnp.float32)] * 4
        low = [jnp.zeros((8, 128), jnp.float32)] * 4
        at = pl.multiple_of(24 * g, 8)
        for s in range(1 + EXTRAS):
            tiles = [
                acc[pl.ds(at + 8 * v, 8), :] if s == 0 else acc_extra[s - 1, pl.ds(at + 8 * v, 8), :]
                for v in range(3)
            ]
            top_r = tiles[0][:, :128] - tiles[1][:, 128:]
            top_i = tiles[0][:, 128:] + tiles[1][:, :128]
            low_r = tiles[2][:, :128] - pltpu.roll(tiles[2][:, 128:], 4, 0)
            low_i = tiles[2][:, 128:] + pltpu.roll(tiles[2][:, :128], 4, 0)
            for b in range(4):
                w_r = weights[8 * s + b : 8 * s + b + 1, :]
                w_i = weights[8 * s + 4 + b : 8 * s + 5 + b, :]
                top[b] = top[b] + (w_r * top_r - w_i * top_i)
                low[b] = low[b] + (w_r * low_r - w_i * low_i)
        low_a = jnp.where(upper, low[0], pltpu.roll(low[1], 4, 0))
        low_b = jnp.where(upper, low[2], pltpu.roll(low[3], 4, 0))
        return jnp.concatenate(top + [low_a, low_b], axis=0)

    core = picks[3]

    def both(z, carry):
        kept[z] = decode(2 * z + core)
        sent[z] = decode(2 * z + 1 - core)
        return carry

    lax.fori_loop(0, PAIRS // 2, both, 0)


def late_product(picks, weights, share, spread, before, early, late):
    return pl.pallas_call(
        late_kernel,
        out_shape=(jax.ShapeDtypeStruct((PAIRS // 2, 48, 128), jnp.float32),) * 2,
        in_specs=[pl.BlockSpec(memory_space=pltpu.SMEM), pl.BlockSpec(memory_space=pltpu.VMEM)]
        + [pl.BlockSpec(memory_space=pl.ANY)] * 11,
        out_specs=(pl.BlockSpec(memory_space=pltpu.VMEM),) * 2,
        scratch_shapes=[
            pltpu.VMEM((ROWS, 256), jnp.float32),
            pltpu.VMEM((2, 512, 256), jnp.bfloat16),
            pltpu.VMEM((EXTRAS, 512, 128), jnp.bfloat16),
            pltpu.VMEM((6, QUADS, 80, 128), jnp.bfloat16),
            pltpu.VMEM((2, QUADS, CHUNK_ROWS, 128), jnp.bfloat16),
            pltpu.VMEM((256, 1152), jnp.float32),
            pltpu.VMEM((EXTRAS, ROWS, 256), jnp.float32),
            pltpu.VMEM((512, 128), jnp.float32),
            pltpu.SemaphoreType.DMA((14,)),
        ],
        name="late_product",
        interpret=INTERPRET,
    )(picks, weights, share, spread, before, *early, *late)


def summed(received):
    total = jnp.sum(received, axis=0)
    top = total[:32].reshape(2, 2, 8, 128)
    low = total[32:].reshape(2, 2, 4, 128)
    return jnp.concatenate([top, low], axis=2).transpose(0, 2, 1, 3)


def shards(source_matrix_tiles, second_operand_encoded, responding_nodes):
    group = ("z", "core")
    sent, picks = encode(
        responding_nodes,
        jnp.asarray(trig_table().reshape(-1)),
        source_matrix_tiles.reshape(96, 128),
    )
    got = lax.all_to_all(sent, group, split_axis=0, concat_axis=0, tiled=True)

    odd = second_operand_encoded[1].reshape(PANELS, PAIRS, 8, 2, 128).transpose(1, 0, 2, 3, 4)
    odd, got = lax.optimization_barrier((odd, got))
    spread = lax.all_to_all(odd, group, split_axis=0, concat_axis=0, tiled=True)
    a = lax.all_gather(compact(got), "quad")

    def hop(chunk, axis, size, by):
        return lax.ppermute(chunk, axis, [(i, (i + by) % size) for i in range(size)])

    y_axes = ("quad", "parity")
    nodes, whole, a = lax.optimization_barrier((responding_nodes, second_operand_encoded, a))
    right_a = hop(a, "x", XS, 1)
    left_a = hop(a, "x", XS, -1)
    b = hop(a, y_axes, YS, -1)
    right_b = hop(right_a, y_axes, YS, 1)
    left_b = hop(left_a, y_axes, YS, -1)
    far_a = hop(right_a, "x", XS, 1)
    far_b = hop(left_b, "x", XS, -1)
    share = split_share(picks, whole.reshape(2, 8192, 128))
    weights = decode_weights(nodes, picks)
    early = (a, b, right_a, left_a, right_b, left_b)
    before = early_product(picks, share, early)
    kept, passed = late_product(
        picks, weights, share, spread.reshape(PAIRS, 512, 128), before, early, (far_a, far_b)
    )
    kept = kept + lax.ppermute(passed, "core", [(0, 1), (1, 0)])
    received = lax.all_to_all(kept, "z", split_axis=0, concat_axis=0, tiled=True)
    return summed(received)


def solution(mesh):
    torus = Mesh(
        mesh.devices.reshape(PAIRS // 2, 2, XS, QUADS, 2), ("z", "core", "x", "quad", "parity")
    )
    group = ("z", "core")
    panel = ("x", "quad", "parity")
    return jax.shard_map(
        shards,
        mesh=torus,
        in_specs=(P(None, group, None, panel), P(group, None, None, panel), P()),
        out_specs=P(None, group, None, panel),
        check_vma=False,
    )
```

```python
import math

import jax
import jax.numpy as jnp
import numpy as np
from jax import lax
from jax.experimental import pallas as pl
from jax.experimental.pallas import tpu as pltpu
from jax.sharding import Mesh
from jax.sharding import PartitionSpec as P


NODE_NUMBER = 32
PAIRS = 16
EXTRAS = 3
XS = 4
YS = 8
QUADS = YS // 2
PANELS = XS * YS
ROWS = 384
CHUNK_ROWS = 464
INTERPRET = False

TWO_PI_RADIANS = 2.0 * math.pi


def trig_table():
    exponent = np.arange(4, dtype=np.float32)[None, :] + 8 * np.arange(2, dtype=np.float32)[:, None]
    point = np.arange(NODE_NUMBER, dtype=np.float32)
    phase = np.float32(TWO_PI_RADIANS) * point / np.float32(NODE_NUMBER)
    angle = (phase[:, None, None] * exponent[None]).astype(np.float64)
    table = np.stack([np.cos(angle), np.sin(angle)], axis=1)
    return table.reshape(NODE_NUMBER, 16).astype(np.float32)


def grid_table():
    grid = np.float32(TWO_PI_RADIANS) * np.arange(NODE_NUMBER, dtype=np.float32) / np.float32(NODE_NUMBER)
    wanted = (3 + 4 * np.arange(4)).astype(np.float32)
    turns = (-grid[None, :] * wanted[:, None]).astype(np.float64)
    grid = grid.astype(np.float64)
    rows = np.zeros((16, 128), np.float32)
    rows[0, :NODE_NUMBER] = np.cos(grid)
    rows[1, :NODE_NUMBER] = np.sin(grid)
    rows[2:6, :NODE_NUMBER] = np.cos(turns)
    rows[6:10, :NODE_NUMBER] = np.sin(turns)
    return rows


def weights_kernel(nodes, picks, points, grid, out):
    number = nodes.shape[0]
    shape = (24, 128)
    row = lax.broadcasted_iota(jnp.int32, shape, 0)
    lane = lax.broadcasted_iota(jnp.int32, shape, 1)
    real = jnp.ones(shape, jnp.float32)
    imag = jnp.zeros(shape, jnp.float32)
    node = jnp.full(shape, -1, jnp.int32)
    for t in range(number):
        mine = row == t
        node = jnp.where(mine, nodes[t], node)
        step_r = jnp.where(mine, 1.0, grid[0:1, :] - points[nodes[t]])
        step_i = jnp.where(mine, 0.0, grid[1:2, :] - points[NODE_NUMBER + nodes[t]])
        real, imag = real * step_r - imag * step_i, real * step_i + imag * step_r

    def across(value):
        return jnp.sum(value, axis=1, keepdims=True)

    here = node == lane
    denom_r = across(jnp.where(here, real, 0.0))
    denom_i = across(jnp.where(here, imag, 0.0))
    magnitude = denom_r * denom_r + denom_i * denom_i
    for e in range(4):
        cos, sin = grid[2 + e : 3 + e, :], grid[6 + e : 7 + e, :]
        numer_r = across(real * cos - imag * sin) / NODE_NUMBER
        numer_i = across(real * sin + imag * cos) / NODE_NUMBER
        weight_r = (numer_r * denom_r + numer_i * denom_i) / magnitude
        weight_i = (numer_i * denom_r - numer_r * denom_i) / magnitude
        for c in range(1 + EXTRAS):
            chosen = node == picks[8 + c]
            out[8 * c + e : 8 * c + e + 1, :] = jnp.sum(
                jnp.where(chosen, weight_r, 0.0), axis=0, keepdims=True
            )
            out[8 * c + 4 + e : 8 * c + 5 + e, :] = jnp.sum(
                jnp.where(chosen, weight_i, 0.0), axis=0, keepdims=True
            )


def decode_weights(nodes, picks):
    grid = grid_table()
    points = grid[:2, :NODE_NUMBER].reshape(-1)
    return pl.pallas_call(
        weights_kernel,
        out_shape=jax.ShapeDtypeStruct((32, 128), jnp.float32),
        in_specs=[pl.BlockSpec(memory_space=pltpu.SMEM)] * 3 + [pl.BlockSpec(memory_space=pltpu.VMEM)],
        out_specs=pl.BlockSpec(memory_space=pltpu.VMEM),
        name="weights",
        interpret=INTERPRET,
    )(nodes, picks, jnp.asarray(points), jnp.asarray(grid))


def position():
    group = 2 * lax.axis_index("z") + lax.axis_index("core")
    return group, lax.axis_index("x"), lax.axis_index("parity")


def encode_kernel(nodes, table, source, out, picks, flags, extra_points, rows, stack):
    for j in range(NODE_NUMBER):
        flags[j] = 0
    for s in range(nodes.shape[0]):
        flags[nodes[s]] = 1
    found = jnp.int32(0)
    for g in range(PAIRS):
        extra_points[found] = 2 * g + 1
        found = found + flags[2 * g] * flags[2 * g + 1]
    group, x, parity = position()
    second = 1 - flags[2 * group]
    picks[0] = second
    picks[1] = x
    picks[2] = parity
    picks[3] = group % 2
    picks[8] = 2 * group + second
    for e in range(EXTRAS):
        picks[4 + e] = (extra_points[e] - 1) // 2
        picks[9 + e] = extra_points[e]

    rows[...] = source[...].astype(jnp.float32)
    tops = []
    lows = []
    for b in range(8):
        at = 48 * (b // 4) + b % 4
        tops.append(rows[pl.ds(at, 8, stride=4), :])
        low = rows[pl.ds(at + 32, 4, stride=4), :]
        lows.append(jnp.concatenate([low, low], axis=0))
    upper = lax.broadcasted_iota(jnp.int32, (8, 128), 0) < 4

    def block(point):
        at = 16 * point
        real = [table[at + b] for b in range(8)]
        imag = [table[at + 8 + b] for b in range(8)]
        top_r = sum(real[b] * tops[b] for b in range(8))
        top_i = sum(imag[b] * tops[b] for b in range(8))
        low = sum(jnp.where(upper, real[b], imag[b]) * lows[b] for b in range(8))
        return [top_r, top_i, low]

    stack[...] = jnp.zeros_like(stack)
    for e in range(EXTRAS):
        for v, tile in enumerate(block(extra_points[e])):
            stack[24 * e + 8 * v : 24 * e + 8 * v + 8, :] = tile
    stack[...] = stack[...].T

    def main(t, carry):
        parts = block(2 * t + 1 - flags[2 * t])
        parts.append(stack[pl.ds(pl.multiple_of(8 * t, 8), 8), :])
        value = jnp.concatenate(parts, axis=0).astype(jnp.bfloat16)
        out[t] = value
        return carry

    lax.fori_loop(0, PAIRS, main, 0)


def encode(nodes, table, source):
    return pl.pallas_call(
        encode_kernel,
        out_shape=(
            jax.ShapeDtypeStruct((PAIRS, 32, 128), jnp.bfloat16),
            jax.ShapeDtypeStruct((16,), jnp.int32),
        ),
        in_specs=[pl.BlockSpec(memory_space=pltpu.SMEM)] * 2 + [pl.BlockSpec(memory_space=pltpu.VMEM)],
        out_specs=(pl.BlockSpec(memory_space=pltpu.VMEM), pl.BlockSpec(memory_space=pltpu.SMEM)),
        scratch_shapes=[
            pltpu.SMEM((NODE_NUMBER,), jnp.int32),
            pltpu.SMEM((PAIRS,), jnp.int32),
            pltpu.VMEM((96, 128), jnp.float32),
            pltpu.VMEM((128, 128), jnp.float32),
        ],
        name="encode",
        interpret=INTERPRET,
    )(nodes, table, source)


def compact_kernel(got, out, rows):
    lane = lax.broadcasted_iota(jnp.int32, (8, 128), 1)
    rows[ROWS + 72 :, :] = jnp.zeros((8, 128), jnp.float32)
    pieces = []
    for g in range(PAIRS):
        block = got[g].astype(jnp.float32)
        rows[24 * g : 24 * g + 24, :] = block[:24]
        pieces.append(block[24:])
    for e in range(EXTRAS):
        for v in range(3):
            tile = jnp.zeros((8, 128), jnp.float32)
            for g in range(PAIRS):
                start = 24 * g - 128 * v
                if start + 24 <= 0 or start >= 128:
                    continue
                moved = pltpu.roll(pieces[g], (start - 24 * e) % 128, 1)
                tile = jnp.where((lane >= start) & (lane < start + 24), moved, tile)
            at = ROWS + 8 * (3 * e + v)
            rows[at : at + 8, :] = tile
    out[...] = rows[...].astype(jnp.bfloat16)


def compact(got):
    return pl.pallas_call(
        compact_kernel,
        out_shape=jax.ShapeDtypeStruct((CHUNK_ROWS, 128), jnp.bfloat16),
        in_specs=[pl.BlockSpec(memory_space=pltpu.VMEM)],
        out_specs=pl.BlockSpec(memory_space=pltpu.VMEM),
        scratch_shapes=[pltpu.VMEM((CHUNK_ROWS, 128), jnp.float32)],
        name="compact",
        interpret=INTERPRET,
    )(got)


def split_pairs(pairs, scratch):
    count = pairs.shape[0] // 2
    scratch[: 2 * count, :] = pairs.astype(jnp.float32)
    real = scratch[pl.ds(0, count, stride=2), :]
    imag = scratch[pl.ds(1, count, stride=2), :]
    return jnp.concatenate([real, imag], axis=1).astype(jnp.bfloat16)


def slices_kernel(picks, spread, out, small, scratch, sems):
    copies = [
        pltpu.make_async_copy(spread.at[picks[4 + e]], small.at[e], sems.at[e]) for e in range(EXTRAS)
    ]
    for copy in copies:
        copy.start()
    for e in range(EXTRAS):
        copies[e].wait()
        out[e] = split_pairs(small[e], scratch)


def split_slices(picks, spread):
    return pl.pallas_call(
        slices_kernel,
        out_shape=jax.ShapeDtypeStruct((EXTRAS, 256, 256), jnp.bfloat16),
        in_specs=[pl.BlockSpec(memory_space=pltpu.SMEM), pl.BlockSpec(memory_space=pl.ANY)],
        out_specs=pl.BlockSpec(memory_space=pltpu.VMEM),
        scratch_shapes=[
            pltpu.VMEM((EXTRAS, 512, 128), jnp.bfloat16),
            pltpu.VMEM((512, 128), jnp.float32),
            pltpu.SemaphoreType.DMA((EXTRAS,)),
        ],
        name="split_slices",
        interpret=INTERPRET,
    )(picks, spread)


def share_kernel(picks, share, out, scratch):
    for y in range(YS):
        piece = split_pairs(share[0, 256 * y : 256 * y + 256, :], scratch)
        out[0, y % 2, 128 * (y // 2) : 128 * (y // 2) + 128, :] = piece


def split_share(picks, share):
    return pl.pallas_call(
        share_kernel,
        out_shape=jax.ShapeDtypeStruct((XS, 2, 512, 256), jnp.bfloat16),
        grid_spec=pltpu.PrefetchScalarGridSpec(
            num_scalar_prefetch=1,
            grid=(XS,),
            in_specs=[pl.BlockSpec((1, 2048, 128), lambda k, picks: (picks[0], k, 0))],
            out_specs=pl.BlockSpec((1, 2, 512, 256), lambda k, picks: (k, 0, 0, 0)),
            scratch_shapes=[pltpu.VMEM((256, 128), jnp.float32)],
        ),
        name="split_share",
        cost_estimate=pl.CostEstimate(flops=400_000_000, bytes_accessed=4_200_000, transcendentals=0),
        interpret=INTERPRET,
    )(picks, share)


def wide(chunk):
    return jnp.concatenate([chunk[q, :ROWS, :] for q in range(QUADS)], axis=1)


def dot(a, b):
    return jnp.dot(a, b, preferred_element_type=jnp.float32)


EARLY = ((0, True), (0, False), (-1, True), (1, True), (-1, False), (1, False))
LATE = ((2, True), (2, False))


def block_of(picks, kind):
    offset, same = kind
    x = (picks[1] + offset + XS) % XS
    return x, picks[2] if same else 1 - picks[2]


def early_kernel(picks, share, c0, c1, c2, c3, c4, c5, acc):
    for n, (chunk, kind) in enumerate(zip((c0, c1, c2, c3, c4, c5), EARLY)):
        x, parity = block_of(picks, kind)
        term = dot(wide(chunk), share[x, parity])
        if n == 0:
            acc[...] = term
        else:
            acc[...] += term


def early_product(picks, share, chunks):
    return pl.pallas_call(
        early_kernel,
        out_shape=jax.ShapeDtypeStruct((ROWS, 256), jnp.float32),
        in_specs=[pl.BlockSpec(memory_space=pltpu.SMEM)] + [pl.BlockSpec(memory_space=pltpu.VMEM)] * 7,
        out_specs=pl.BlockSpec(memory_space=pltpu.VMEM),
        name="early_product",
        cost_estimate=pl.CostEstimate(flops=400_000_000, bytes_accessed=4_200_000, transcendentals=0),
        interpret=INTERPRET,
    )(picks, share, *chunks)


def late_kernel(
    picks, weights, share, slices, before, c0, c1, c2, c3, c4, c5, c6, c7, kept, sent,
    acc, blocks, small, ends, late, extra, acc_extra, sems,
):
    early = (c0, c1, c2, c3, c4, c5)
    chunks = (c6, c7)
    copies = []

    def start(source, target):
        copy = pltpu.make_async_copy(source, target, sems.at[len(copies)])
        copy.start()
        copies.append(copy)

    start(slices, small)
    for n in range(6):
        start(early[n].at[:, pl.ds(ROWS, 80), :], ends.at[n])
    for n in range(2):
        x, parity = block_of(picks, LATE[n])
        start(chunks[n], late.at[n])
        start(share.at[x, parity], blocks.at[n])
    start(before, acc)

    def place(rows_of, kind):
        x, parity = block_of(picks, kind)
        for q in range(QUADS):
            rows = rows_of(q)
            at = pl.multiple_of(8 * (YS * x + 2 * q + parity), 8)
            for v in range(9):
                extra[pl.ds(at, 8), 128 * v : 128 * v + 128] = rows[8 * v : 8 * v + 8]

    for copy in copies[:7]:
        copy.wait()
    for n in range(6):
        place(lambda q: ends[n, q].astype(jnp.float32), EARLY[n])
    for n in range(2):
        copies[7 + 2 * n].wait()
        place(lambda q: late[n, q, ROWS:, :].astype(jnp.float32), LATE[n])
    for e in range(EXTRAS):
        turned = extra[:, ROWS * e : ROWS * e + ROWS].astype(jnp.bfloat16)
        acc_extra[e] = lax.dot_general(
            turned, small[e], (((0,), (0,)), ((), ())), preferred_element_type=jnp.float32
        )
    copies[11].wait()
    for n in range(2):
        copies[8 + 2 * n].wait()
        acc[...] += dot(wide(late.at[n]), blocks[n])

    upper = lax.broadcasted_iota(jnp.int32, (8, 128), 0) < 4

    def decode(g):
        top = [jnp.zeros((8, 128), jnp.float32)] * 4
        low = [jnp.zeros((8, 128), jnp.float32)] * 4
        at = pl.multiple_of(24 * g, 8)
        for s in range(1 + EXTRAS):
            tiles = [
                acc[pl.ds(at + 8 * v, 8), :] if s == 0 else acc_extra[s - 1, pl.ds(at + 8 * v, 8), :]
                for v in range(3)
            ]
            top_r = tiles[0][:, :128] - tiles[1][:, 128:]
            top_i = tiles[0][:, 128:] + tiles[1][:, :128]
            low_r = tiles[2][:, :128] - pltpu.roll(tiles[2][:, 128:], 4, 0)
            low_i = tiles[2][:, 128:] + pltpu.roll(tiles[2][:, :128], 4, 0)
            for b in range(4):
                w_r = weights[8 * s + b : 8 * s + b + 1, :]
                w_i = weights[8 * s + 4 + b : 8 * s + 5 + b, :]
                top[b] = top[b] + (w_r * top_r - w_i * top_i)
                low[b] = low[b] + (w_r * low_r - w_i * low_i)
        low_a = jnp.where(upper, low[0], pltpu.roll(low[1], 4, 0))
        low_b = jnp.where(upper, low[2], pltpu.roll(low[3], 4, 0))
        return jnp.concatenate(top + [low_a, low_b], axis=0)

    core = picks[3]

    def both(z, carry):
        kept[z] = decode(2 * z + core)
        sent[z] = decode(2 * z + 1 - core)
        return carry

    lax.fori_loop(0, PAIRS // 2, both, 0)


def late_product(picks, weights, share, slices, before, early, late):
    return pl.pallas_call(
        late_kernel,
        out_shape=(jax.ShapeDtypeStruct((PAIRS // 2, 48, 128), jnp.float32),) * 2,
        in_specs=[pl.BlockSpec(memory_space=pltpu.SMEM), pl.BlockSpec(memory_space=pltpu.VMEM)]
        + [pl.BlockSpec(memory_space=pl.ANY)] * 11,
        out_specs=(pl.BlockSpec(memory_space=pltpu.VMEM),) * 2,
        scratch_shapes=[
            pltpu.VMEM((ROWS, 256), jnp.float32),
            pltpu.VMEM((2, 512, 256), jnp.bfloat16),
            pltpu.VMEM((EXTRAS, 256, 256), jnp.bfloat16),
            pltpu.VMEM((6, QUADS, 80, 128), jnp.bfloat16),
            pltpu.VMEM((2, QUADS, CHUNK_ROWS, 128), jnp.bfloat16),
            pltpu.VMEM((256, 1152), jnp.float32),
            pltpu.VMEM((EXTRAS, ROWS, 256), jnp.float32),
            pltpu.SemaphoreType.DMA((12,)),
        ],
        name="late_product",
        interpret=INTERPRET,
    )(picks, weights, share, slices, before, *early, *late)


def summed(received):
    total = jnp.sum(received, axis=0)
    top = total[:32].reshape(2, 2, 8, 128)
    low = total[32:].reshape(2, 2, 4, 128)
    return jnp.concatenate([top, low], axis=2).transpose(0, 2, 1, 3)


def shards(source_matrix_tiles, second_operand_encoded, responding_nodes):
    group = ("z", "core")
    sent, picks = encode(
        responding_nodes,
        jnp.asarray(trig_table().reshape(-1)),
        source_matrix_tiles.reshape(96, 128),
    )
    got = lax.all_to_all(sent, group, split_axis=0, concat_axis=0, tiled=True)

    odd = second_operand_encoded[1].reshape(PANELS, PAIRS, 8, 2, 128).transpose(1, 0, 2, 3, 4)
    odd, got = lax.optimization_barrier((odd, got))
    spread = lax.all_to_all(odd, group, split_axis=0, concat_axis=0, tiled=True)
    a = lax.all_gather(compact(got), "quad")

    def hop(chunk, axis, size, by):
        return lax.ppermute(chunk, axis, [(i, (i + by) % size) for i in range(size)])

    y_axes = ("quad", "parity")
    nodes, whole, a = lax.optimization_barrier((responding_nodes, second_operand_encoded, a))
    right_a = hop(a, "x", XS, 1)
    left_a = hop(a, "x", XS, -1)
    b = hop(a, y_axes, YS, 1)
    right_b = hop(right_a, y_axes, YS, 1)
    left_b = hop(left_a, y_axes, YS, -1)
    far_a = hop(right_a, "x", XS, 1)
    far_b = hop(left_b, "x", XS, -1)
    share = split_share(picks, whole.reshape(2, 8192, 128))
    weights = decode_weights(nodes, picks)
    early = (a, b, right_a, left_a, right_b, left_b)
    before = early_product(picks, share, early)
    slices = split_slices(picks, spread.reshape(PAIRS, 512, 128))
    kept, passed = late_product(
        picks, weights, share, slices, before, early, (far_a, far_b)
    )
    kept = kept + lax.ppermute(passed, "core", [(0, 1), (1, 0)])
    received = lax.all_to_all(kept, "z", split_axis=0, concat_axis=0, tiled=True)
    return summed(received)


def solution(mesh):
    torus = Mesh(
        mesh.devices.reshape(PAIRS // 2, 2, XS, QUADS, 2), ("z", "core", "x", "quad", "parity")
    )
    group = ("z", "core")
    panel = ("x", "quad", "parity")
    return jax.shard_map(
        shards,
        mesh=torus,
        in_specs=(P(None, group, None, panel), P(group, None, None, panel), P()),
        out_specs=P(None, group, None, panel),
        check_vma=False,
    )
```

```python
import math

import jax
import jax.numpy as jnp
import numpy as np
from jax import lax
from jax.experimental import pallas as pl
from jax.experimental.pallas import tpu as pltpu
from jax.sharding import Mesh
from jax.sharding import PartitionSpec as P


NODE_NUMBER = 32
PAIRS = 16
EXTRAS = 3
XS = 4
YS = 8
QUADS = YS // 2
PANELS = XS * YS
ROWS = 384
CHUNK_ROWS = 464
INTERPRET = False

TWO_PI_RADIANS = 2.0 * math.pi


def trig_table():
    exponent = np.arange(4, dtype=np.float32)[None, :] + 8 * np.arange(2, dtype=np.float32)[:, None]
    point = np.arange(NODE_NUMBER, dtype=np.float32)
    phase = np.float32(TWO_PI_RADIANS) * point / np.float32(NODE_NUMBER)
    angle = (phase[:, None, None] * exponent[None]).astype(np.float64)
    table = np.stack([np.cos(angle), np.sin(angle)], axis=1)
    return table.reshape(NODE_NUMBER, 16).astype(np.float32)


def grid_table():
    grid = np.float32(TWO_PI_RADIANS) * np.arange(NODE_NUMBER, dtype=np.float32) / np.float32(NODE_NUMBER)
    wanted = (3 + 4 * np.arange(4)).astype(np.float32)
    turns = (-grid[None, :] * wanted[:, None]).astype(np.float64)
    grid = grid.astype(np.float64)
    rows = np.zeros((16, 128), np.float32)
    rows[0, :NODE_NUMBER] = np.cos(grid)
    rows[1, :NODE_NUMBER] = np.sin(grid)
    rows[2:6, :NODE_NUMBER] = np.cos(turns)
    rows[6:10, :NODE_NUMBER] = np.sin(turns)
    return rows


def weights_kernel(nodes, picks, points, grid, out):
    number = nodes.shape[0]
    shape = (24, 128)
    row = lax.broadcasted_iota(jnp.int32, shape, 0)
    lane = lax.broadcasted_iota(jnp.int32, shape, 1)
    real = jnp.ones(shape, jnp.float32)
    imag = jnp.zeros(shape, jnp.float32)
    node = jnp.full(shape, -1, jnp.int32)
    for t in range(number):
        mine = row == t
        node = jnp.where(mine, nodes[t], node)
        step_r = jnp.where(mine, 1.0, grid[0:1, :] - points[nodes[t]])
        step_i = jnp.where(mine, 0.0, grid[1:2, :] - points[NODE_NUMBER + nodes[t]])
        real, imag = real * step_r - imag * step_i, real * step_i + imag * step_r

    def across(value):
        return jnp.sum(value, axis=1, keepdims=True)

    here = node == lane
    denom_r = across(jnp.where(here, real, 0.0))
    denom_i = across(jnp.where(here, imag, 0.0))
    magnitude = denom_r * denom_r + denom_i * denom_i
    for e in range(4):
        cos, sin = grid[2 + e : 3 + e, :], grid[6 + e : 7 + e, :]
        numer_r = across(real * cos - imag * sin) / NODE_NUMBER
        numer_i = across(real * sin + imag * cos) / NODE_NUMBER
        weight_r = (numer_r * denom_r + numer_i * denom_i) / magnitude
        weight_i = (numer_i * denom_r - numer_r * denom_i) / magnitude
        for c in range(1 + EXTRAS):
            chosen = node == picks[8 + c]
            out[8 * c + e : 8 * c + e + 1, :] = jnp.sum(
                jnp.where(chosen, weight_r, 0.0), axis=0, keepdims=True
            )
            out[8 * c + 4 + e : 8 * c + 5 + e, :] = jnp.sum(
                jnp.where(chosen, weight_i, 0.0), axis=0, keepdims=True
            )


def decode_weights(nodes, picks):
    grid = grid_table()
    points = grid[:2, :NODE_NUMBER].reshape(-1)
    return pl.pallas_call(
        weights_kernel,
        out_shape=jax.ShapeDtypeStruct((32, 128), jnp.float32),
        in_specs=[pl.BlockSpec(memory_space=pltpu.SMEM)] * 3 + [pl.BlockSpec(memory_space=pltpu.VMEM)],
        out_specs=pl.BlockSpec(memory_space=pltpu.VMEM),
        name="weights",
        interpret=INTERPRET,
    )(nodes, picks, jnp.asarray(points), jnp.asarray(grid))


def position():
    group = 2 * lax.axis_index("z") + lax.axis_index("core")
    return group, lax.axis_index("x"), lax.axis_index("parity")


def encode_kernel(nodes, table, source, out, picks, flags, extra_points, rows, stack):
    for j in range(NODE_NUMBER):
        flags[j] = 0
    for s in range(nodes.shape[0]):
        flags[nodes[s]] = 1
    found = jnp.int32(0)
    for g in range(PAIRS):
        extra_points[found] = 2 * g + 1
        found = found + flags[2 * g] * flags[2 * g + 1]
    group, x, parity = position()
    second = 1 - flags[2 * group]
    picks[0] = second
    picks[1] = x
    picks[2] = parity
    picks[3] = group % 2
    picks[8] = 2 * group + second
    for e in range(EXTRAS):
        picks[4 + e] = (extra_points[e] - 1) // 2
        picks[9 + e] = extra_points[e]

    rows[...] = source[...].astype(jnp.float32)
    tops = []
    lows = []
    for b in range(8):
        at = 48 * (b // 4) + b % 4
        tops.append(rows[pl.ds(at, 8, stride=4), :])
        low = rows[pl.ds(at + 32, 4, stride=4), :]
        lows.append(jnp.concatenate([low, low], axis=0))
    upper = lax.broadcasted_iota(jnp.int32, (8, 128), 0) < 4

    def block(point):
        at = 16 * point
        real = [table[at + b] for b in range(8)]
        imag = [table[at + 8 + b] for b in range(8)]
        top_r = sum(real[b] * tops[b] for b in range(8))
        top_i = sum(imag[b] * tops[b] for b in range(8))
        low = sum(jnp.where(upper, real[b], imag[b]) * lows[b] for b in range(8))
        return [top_r, top_i, low]

    stack[...] = jnp.zeros_like(stack)
    for e in range(EXTRAS):
        for v, tile in enumerate(block(extra_points[e])):
            stack[24 * e + 8 * v : 24 * e + 8 * v + 8, :] = tile
    stack[...] = stack[...].T

    def main(t, carry):
        parts = block(2 * t + 1 - flags[2 * t])
        parts.append(stack[pl.ds(pl.multiple_of(8 * t, 8), 8), :])
        value = jnp.concatenate(parts, axis=0).astype(jnp.bfloat16)
        out[t] = value
        return carry

    lax.fori_loop(0, PAIRS, main, 0)


def encode(nodes, table, source):
    return pl.pallas_call(
        encode_kernel,
        out_shape=(
            jax.ShapeDtypeStruct((PAIRS, 32, 128), jnp.bfloat16),
            jax.ShapeDtypeStruct((16,), jnp.int32),
        ),
        in_specs=[pl.BlockSpec(memory_space=pltpu.SMEM)] * 2 + [pl.BlockSpec(memory_space=pltpu.VMEM)],
        out_specs=(pl.BlockSpec(memory_space=pltpu.VMEM), pl.BlockSpec(memory_space=pltpu.SMEM)),
        scratch_shapes=[
            pltpu.SMEM((NODE_NUMBER,), jnp.int32),
            pltpu.SMEM((PAIRS,), jnp.int32),
            pltpu.VMEM((96, 128), jnp.float32),
            pltpu.VMEM((128, 128), jnp.float32),
        ],
        name="encode",
        interpret=INTERPRET,
    )(nodes, table, source)


def compact_kernel(got, out, rows):
    lane = lax.broadcasted_iota(jnp.int32, (8, 128), 1)
    rows[ROWS + 72 :, :] = jnp.zeros((8, 128), jnp.float32)
    pieces = []
    for g in range(PAIRS):
        block = got[g].astype(jnp.float32)
        rows[24 * g : 24 * g + 24, :] = block[:24]
        pieces.append(block[24:])
    for e in range(EXTRAS):
        for v in range(3):
            tile = jnp.zeros((8, 128), jnp.float32)
            for g in range(PAIRS):
                start = 24 * g - 128 * v
                if start + 24 <= 0 or start >= 128:
                    continue
                moved = pltpu.roll(pieces[g], (start - 24 * e) % 128, 1)
                tile = jnp.where((lane >= start) & (lane < start + 24), moved, tile)
            at = ROWS + 8 * (3 * e + v)
            rows[at : at + 8, :] = tile
    out[...] = rows[...].astype(jnp.bfloat16)


def compact(got):
    return pl.pallas_call(
        compact_kernel,
        out_shape=jax.ShapeDtypeStruct((CHUNK_ROWS, 128), jnp.bfloat16),
        in_specs=[pl.BlockSpec(memory_space=pltpu.VMEM)],
        out_specs=pl.BlockSpec(memory_space=pltpu.VMEM),
        scratch_shapes=[pltpu.VMEM((CHUNK_ROWS, 128), jnp.float32)],
        name="compact",
        interpret=INTERPRET,
    )(got)


def split_pairs(pairs, scratch):
    count = pairs.shape[0] // 2
    scratch[: 2 * count, :] = pairs.astype(jnp.float32)
    real = scratch[pl.ds(0, count, stride=2), :]
    imag = scratch[pl.ds(1, count, stride=2), :]
    return jnp.concatenate([real, imag], axis=1).astype(jnp.bfloat16)


def share_kernel(picks, share, out, scratch):
    for y in range(YS):
        piece = split_pairs(share[0, 256 * y : 256 * y + 256, :], scratch)
        out[0, y % 2, 128 * (y // 2) : 128 * (y // 2) + 128, :] = piece


def split_share(picks, share):
    return pl.pallas_call(
        share_kernel,
        out_shape=jax.ShapeDtypeStruct((XS, 2, 512, 256), jnp.bfloat16),
        grid_spec=pltpu.PrefetchScalarGridSpec(
            num_scalar_prefetch=1,
            grid=(XS,),
            in_specs=[pl.BlockSpec((1, 2048, 128), lambda k, picks: (picks[0], k, 0))],
            out_specs=pl.BlockSpec((1, 2, 512, 256), lambda k, picks: (k, 0, 0, 0)),
            scratch_shapes=[pltpu.VMEM((256, 128), jnp.float32)],
        ),
        name="split_share",
        cost_estimate=pl.CostEstimate(flops=400_000_000, bytes_accessed=4_200_000, transcendentals=0),
        interpret=INTERPRET,
    )(picks, share)


def wide(chunk):
    return jnp.concatenate([chunk[q, :ROWS, :] for q in range(QUADS)], axis=1)


def dot(a, b):
    return jnp.dot(a, b, preferred_element_type=jnp.float32)


EARLY = ((0, True), (0, False), (-1, True), (1, True), (-1, False), (1, False))
LATE = ((2, True), (2, False))


def block_of(picks, kind):
    offset, same = kind
    x = (picks[1] + offset + XS) % XS
    return x, picks[2] if same else 1 - picks[2]


def early_kernel(picks, share, c0, c1, c2, c3, c4, c5, spread, acc):
    for n, (chunk, kind) in enumerate(zip((c0, c1, c2, c3, c4, c5), EARLY)):
        x, parity = block_of(picks, kind)
        term = dot(wide(chunk), share[x, parity])
        if n == 0:
            acc[...] = term
        else:
            acc[...] += term


def early_product(picks, share, chunks, spread):
    return pl.pallas_call(
        early_kernel,
        out_shape=jax.ShapeDtypeStruct((ROWS, 256), jnp.float32),
        in_specs=[pl.BlockSpec(memory_space=pltpu.SMEM)] + [pl.BlockSpec(memory_space=pltpu.VMEM)] * 7
        + [pl.BlockSpec(memory_space=pl.ANY)],
        out_specs=pl.BlockSpec(memory_space=pltpu.VMEM),
        name="early_product",
        cost_estimate=pl.CostEstimate(flops=400_000_000, bytes_accessed=4_200_000, transcendentals=0),
        interpret=INTERPRET,
    )(picks, share, *chunks, spread)


def late_kernel(
    picks, weights, share, spread, before, c0, c1, c2, c3, c4, c5, c6, c7, kept, sent,
    acc, blocks, small, ends, late, extra, acc_extra, scratch, sems,
):
    early = (c0, c1, c2, c3, c4, c5)
    chunks = (c6, c7)
    copies = []

    def start(source, target):
        copy = pltpu.make_async_copy(source, target, sems.at[len(copies)])
        copy.start()
        copies.append(copy)

    for e in range(EXTRAS):
        start(spread.at[picks[4 + e]], small.at[e])
    for n in range(6):
        start(early[n].at[:, pl.ds(ROWS, 80), :], ends.at[n])
    for n in range(2):
        x, parity = block_of(picks, LATE[n])
        start(chunks[n], late.at[n])
        start(share.at[x, parity], blocks.at[n])
    start(before, acc)

    def place(rows_of, kind):
        x, parity = block_of(picks, kind)
        for q in range(QUADS):
            rows = rows_of(q)
            at = pl.multiple_of(8 * (YS * x + 2 * q + parity), 8)
            for v in range(9):
                extra[pl.ds(at, 8), 128 * v : 128 * v + 128] = rows[8 * v : 8 * v + 8]

    for copy in copies[:9]:
        copy.wait()
    for n in range(6):
        place(lambda q: ends[n, q].astype(jnp.float32), EARLY[n])
    slices = [split_pairs(small[e], scratch) for e in range(EXTRAS)]
    for n in range(2):
        copies[9 + 2 * n].wait()
        place(lambda q: late[n, q, ROWS:, :].astype(jnp.float32), LATE[n])
    for e in range(EXTRAS):
        turned = extra[:, ROWS * e : ROWS * e + ROWS].astype(jnp.bfloat16)
        acc_extra[e] = lax.dot_general(
            turned, slices[e], (((0,), (0,)), ((), ())), preferred_element_type=jnp.float32
        )
    copies[13].wait()
    for n in range(2):
        copies[10 + 2 * n].wait()
        acc[...] += dot(wide(late.at[n]), blocks[n])

    upper = lax.broadcasted_iota(jnp.int32, (8, 128), 0) < 4

    def decode(g):
        top = [jnp.zeros((8, 128), jnp.float32)] * 4
        low = [jnp.zeros((8, 128), jnp.float32)] * 4
        at = pl.multiple_of(24 * g, 8)
        for s in range(1 + EXTRAS):
            tiles = [
                acc[pl.ds(at + 8 * v, 8), :] if s == 0 else acc_extra[s - 1, pl.ds(at + 8 * v, 8), :]
                for v in range(3)
            ]
            top_r = tiles[0][:, :128] - tiles[1][:, 128:]
            top_i = tiles[0][:, 128:] + tiles[1][:, :128]
            low_r = tiles[2][:, :128] - pltpu.roll(tiles[2][:, 128:], 4, 0)
            low_i = tiles[2][:, 128:] + pltpu.roll(tiles[2][:, :128], 4, 0)
            for b in range(4):
                w_r = weights[8 * s + b : 8 * s + b + 1, :]
                w_i = weights[8 * s + 4 + b : 8 * s + 5 + b, :]
                top[b] = top[b] + (w_r * top_r - w_i * top_i)
                low[b] = low[b] + (w_r * low_r - w_i * low_i)
        low_a = jnp.where(upper, low[0], pltpu.roll(low[1], 4, 0))
        low_b = jnp.where(upper, low[2], pltpu.roll(low[3], 4, 0))
        return jnp.concatenate(top + [low_a, low_b], axis=0)

    core = picks[3]

    def both(z, carry):
        kept[z] = decode(2 * z + core)
        sent[z] = decode(2 * z + 1 - core)
        return carry

    lax.fori_loop(0, PAIRS // 2, both, 0)


def late_product(picks, weights, share, spread, before, early, late):
    return pl.pallas_call(
        late_kernel,
        out_shape=(jax.ShapeDtypeStruct((PAIRS // 2, 48, 128), jnp.float32),) * 2,
        in_specs=[pl.BlockSpec(memory_space=pltpu.SMEM), pl.BlockSpec(memory_space=pltpu.VMEM)]
        + [pl.BlockSpec(memory_space=pl.ANY)] * 11,
        out_specs=(pl.BlockSpec(memory_space=pltpu.VMEM),) * 2,
        scratch_shapes=[
            pltpu.VMEM((ROWS, 256), jnp.float32),
            pltpu.VMEM((2, 512, 256), jnp.bfloat16),
            pltpu.VMEM((EXTRAS, 512, 128), jnp.bfloat16),
            pltpu.VMEM((6, QUADS, 80, 128), jnp.bfloat16),
            pltpu.VMEM((2, QUADS, CHUNK_ROWS, 128), jnp.bfloat16),
            pltpu.VMEM((256, 1152), jnp.float32),
            pltpu.VMEM((EXTRAS, ROWS, 256), jnp.float32),
            pltpu.VMEM((512, 128), jnp.float32),
            pltpu.SemaphoreType.DMA((14,)),
        ],
        name="late_product",
        interpret=INTERPRET,
    )(picks, weights, share, spread, before, *early, *late)


def summed(received):
    total = jnp.sum(received, axis=0)
    top = total[:32].reshape(2, 2, 8, 128)
    low = total[32:].reshape(2, 2, 4, 128)
    return jnp.concatenate([top, low], axis=2).transpose(0, 2, 1, 3)


def shards(source_matrix_tiles, second_operand_encoded, responding_nodes):
    group = ("z", "core")
    sent, picks = encode(
        responding_nodes,
        jnp.asarray(trig_table().reshape(-1)),
        source_matrix_tiles.reshape(96, 128),
    )
    got = lax.all_to_all(sent, group, split_axis=0, concat_axis=0, tiled=True)

    share = split_share(picks, second_operand_encoded.reshape(2, 8192, 128))

    odd = second_operand_encoded[1].reshape(PANELS, PAIRS, 8, 2, 128).transpose(1, 0, 2, 3, 4)
    odd, got = lax.optimization_barrier((odd, got))
    spread = lax.all_to_all(odd, group, split_axis=0, concat_axis=0, tiled=True)
    a = lax.all_gather(compact(got), "quad")

    def hop(chunk, axis, size, by):
        return lax.ppermute(chunk, axis, [(i, (i + by) % size) for i in range(size)])

    y_axes = ("quad", "parity")
    nodes, a = lax.optimization_barrier((responding_nodes, a))
    right_a = hop(a, "x", XS, 1)
    left_a = hop(a, "x", XS, -1)
    b = hop(a, y_axes, YS, -1)
    right_b = hop(right_a, y_axes, YS, 1)
    left_b = hop(left_a, y_axes, YS, -1)
    far_a = hop(right_a, "x", XS, 1)
    far_b = hop(left_b, "x", XS, -1)
    weights = decode_weights(nodes, picks)
    early = (a, b, right_a, left_a, right_b, left_b)
    spread = spread.reshape(PAIRS, 512, 128)
    before = early_product(picks, share, early, spread)
    kept, passed = late_product(
        picks, weights, share, spread, before, early, (far_a, far_b)
    )
    kept = kept + lax.ppermute(passed, "core", [(0, 1), (1, 0)])
    received = lax.all_to_all(kept, "z", split_axis=0, concat_axis=0, tiled=True)
    return summed(received)


def solution(mesh):
    torus = Mesh(
        mesh.devices.reshape(PAIRS // 2, 2, XS, QUADS, 2), ("z", "core", "x", "quad", "parity")
    )
    group = ("z", "core")
    panel = ("x", "quad", "parity")
    return jax.shard_map(
        shards,
        mesh=torus,
        in_specs=(P(None, group, None, panel), P(group, None, None, panel), P()),
        out_specs=P(None, group, None, panel),
        check_vma=False,
    )
```

```python
import math

import jax
import jax.numpy as jnp
import numpy as np
from jax import lax
from jax.experimental import pallas as pl
from jax.experimental.pallas import tpu as pltpu
from jax.sharding import Mesh
from jax.sharding import PartitionSpec as P


NODE_NUMBER = 32
PAIRS = 16
EXTRAS = 3
XS = 4
YS = 8
QUADS = YS // 2
PANELS = XS * YS
ROWS = 384
CHUNK_ROWS = 464
INTERPRET = False

TWO_PI_RADIANS = 2.0 * math.pi


def trig_table():
    exponent = np.arange(4, dtype=np.float32)[None, :] + 8 * np.arange(2, dtype=np.float32)[:, None]
    point = np.arange(NODE_NUMBER, dtype=np.float32)
    phase = np.float32(TWO_PI_RADIANS) * point / np.float32(NODE_NUMBER)
    angle = (phase[:, None, None] * exponent[None]).astype(np.float64)
    table = np.stack([np.cos(angle), np.sin(angle)], axis=1)
    return table.reshape(NODE_NUMBER, 16).astype(np.float32)


def grid_table():
    grid = np.float32(TWO_PI_RADIANS) * np.arange(NODE_NUMBER, dtype=np.float32) / np.float32(NODE_NUMBER)
    wanted = (3 + 4 * np.arange(4)).astype(np.float32)
    turns = (-grid[None, :] * wanted[:, None]).astype(np.float64)
    grid = grid.astype(np.float64)
    rows = np.zeros((16, 128), np.float32)
    rows[0, :NODE_NUMBER] = np.cos(grid)
    rows[1, :NODE_NUMBER] = np.sin(grid)
    rows[2:6, :NODE_NUMBER] = np.cos(turns)
    rows[6:10, :NODE_NUMBER] = np.sin(turns)
    return rows


def weights_kernel(nodes, picks, points, grid, out):
    number = nodes.shape[0]
    shape = (24, 128)
    row = lax.broadcasted_iota(jnp.int32, shape, 0)
    lane = lax.broadcasted_iota(jnp.int32, shape, 1)
    real = jnp.ones(shape, jnp.float32)
    imag = jnp.zeros(shape, jnp.float32)
    node = jnp.full(shape, -1, jnp.int32)
    for t in range(number):
        mine = row == t
        node = jnp.where(mine, nodes[t], node)
        step_r = jnp.where(mine, 1.0, grid[0:1, :] - points[nodes[t]])
        step_i = jnp.where(mine, 0.0, grid[1:2, :] - points[NODE_NUMBER + nodes[t]])
        real, imag = real * step_r - imag * step_i, real * step_i + imag * step_r

    def across(value):
        return jnp.sum(value, axis=1, keepdims=True)

    here = node == lane
    denom_r = across(jnp.where(here, real, 0.0))
    denom_i = across(jnp.where(here, imag, 0.0))
    magnitude = denom_r * denom_r + denom_i * denom_i
    for e in range(4):
        cos, sin = grid[2 + e : 3 + e, :], grid[6 + e : 7 + e, :]
        numer_r = across(real * cos - imag * sin) / NODE_NUMBER
        numer_i = across(real * sin + imag * cos) / NODE_NUMBER
        weight_r = (numer_r * denom_r + numer_i * denom_i) / magnitude
        weight_i = (numer_i * denom_r - numer_r * denom_i) / magnitude
        for c in range(1 + EXTRAS):
            chosen = node == picks[8 + c]
            out[8 * c + e : 8 * c + e + 1, :] = jnp.sum(
                jnp.where(chosen, weight_r, 0.0), axis=0, keepdims=True
            )
            out[8 * c + 4 + e : 8 * c + 5 + e, :] = jnp.sum(
                jnp.where(chosen, weight_i, 0.0), axis=0, keepdims=True
            )


def decode_weights(nodes, picks):
    grid = grid_table()
    points = grid[:2, :NODE_NUMBER].reshape(-1)
    return pl.pallas_call(
        weights_kernel,
        out_shape=jax.ShapeDtypeStruct((32, 128), jnp.float32),
        in_specs=[pl.BlockSpec(memory_space=pltpu.SMEM)] * 3 + [pl.BlockSpec(memory_space=pltpu.VMEM)],
        out_specs=pl.BlockSpec(memory_space=pltpu.VMEM),
        name="weights",
        interpret=INTERPRET,
    )(nodes, picks, jnp.asarray(points), jnp.asarray(grid))


def position():
    group = 2 * lax.axis_index("z") + lax.axis_index("core")
    return group, lax.axis_index("x"), lax.axis_index("parity")


def encode_kernel(nodes, table, source, out, picks, flags, extra_points, rows, stack):
    for j in range(NODE_NUMBER):
        flags[j] = 0
    for s in range(nodes.shape[0]):
        flags[nodes[s]] = 1
    found = jnp.int32(0)
    for g in range(PAIRS):
        extra_points[found] = 2 * g + 1
        found = found + flags[2 * g] * flags[2 * g + 1]
    group, x, parity = position()
    second = 1 - flags[2 * group]
    picks[0] = second
    picks[1] = x
    picks[2] = parity
    picks[3] = group % 2
    picks[8] = 2 * group + second
    for e in range(EXTRAS):
        picks[4 + e] = (extra_points[e] - 1) // 2
        picks[9 + e] = extra_points[e]

    rows[...] = source[...].astype(jnp.float32)
    tops = []
    lows = []
    for b in range(8):
        at = 48 * (b // 4) + b % 4
        tops.append(rows[pl.ds(at, 8, stride=4), :])
        low = rows[pl.ds(at + 32, 4, stride=4), :]
        lows.append(jnp.concatenate([low, low], axis=0))
    upper = lax.broadcasted_iota(jnp.int32, (8, 128), 0) < 4

    def block(point):
        at = 16 * point
        real = [table[at + b] for b in range(8)]
        imag = [table[at + 8 + b] for b in range(8)]
        top_r = sum(real[b] * tops[b] for b in range(8))
        top_i = sum(imag[b] * tops[b] for b in range(8))
        low = sum(jnp.where(upper, real[b], imag[b]) * lows[b] for b in range(8))
        return [top_r, top_i, low]

    stack[...] = jnp.zeros_like(stack)
    for e in range(EXTRAS):
        for v, tile in enumerate(block(extra_points[e])):
            stack[24 * e + 8 * v : 24 * e + 8 * v + 8, :] = tile
    stack[...] = stack[...].T

    def main(t, carry):
        parts = block(2 * t + 1 - flags[2 * t])
        parts.append(stack[pl.ds(pl.multiple_of(8 * t, 8), 8), :])
        value = jnp.concatenate(parts, axis=0).astype(jnp.bfloat16)
        out[t] = value
        return carry

    lax.fori_loop(0, PAIRS, main, 0)


def encode(nodes, table, source):
    return pl.pallas_call(
        encode_kernel,
        out_shape=(
            jax.ShapeDtypeStruct((PAIRS, 32, 128), jnp.bfloat16),
            jax.ShapeDtypeStruct((16,), jnp.int32),
        ),
        in_specs=[pl.BlockSpec(memory_space=pltpu.SMEM)] * 2 + [pl.BlockSpec(memory_space=pltpu.VMEM)],
        out_specs=(pl.BlockSpec(memory_space=pltpu.VMEM), pl.BlockSpec(memory_space=pltpu.SMEM)),
        scratch_shapes=[
            pltpu.SMEM((NODE_NUMBER,), jnp.int32),
            pltpu.SMEM((PAIRS,), jnp.int32),
            pltpu.VMEM((96, 128), jnp.float32),
            pltpu.VMEM((128, 128), jnp.float32),
        ],
        name="encode",
        interpret=INTERPRET,
    )(nodes, table, source)


def compact_kernel(got, out, rows):
    lane = lax.broadcasted_iota(jnp.int32, (8, 128), 1)
    rows[ROWS + 72 :, :] = jnp.zeros((8, 128), jnp.float32)
    pieces = []
    for g in range(PAIRS):
        block = got[g].astype(jnp.float32)
        rows[24 * g : 24 * g + 24, :] = block[:24]
        pieces.append(block[24:])
    for e in range(EXTRAS):
        for v in range(3):
            tile = jnp.zeros((8, 128), jnp.float32)
            for g in range(PAIRS):
                start = 24 * g - 128 * v
                if start + 24 <= 0 or start >= 128:
                    continue
                moved = pltpu.roll(pieces[g], (start - 24 * e) % 128, 1)
                tile = jnp.where((lane >= start) & (lane < start + 24), moved, tile)
            at = ROWS + 8 * (3 * e + v)
            rows[at : at + 8, :] = tile
    out[...] = rows[...].astype(jnp.bfloat16)


def compact(got):
    return pl.pallas_call(
        compact_kernel,
        out_shape=jax.ShapeDtypeStruct((CHUNK_ROWS, 128), jnp.bfloat16),
        in_specs=[pl.BlockSpec(memory_space=pltpu.VMEM)],
        out_specs=pl.BlockSpec(memory_space=pltpu.VMEM),
        scratch_shapes=[pltpu.VMEM((CHUNK_ROWS, 128), jnp.float32)],
        name="compact",
        interpret=INTERPRET,
    )(got)


def split_pairs(pairs, scratch):
    count = pairs.shape[0] // 2
    scratch[: 2 * count, :] = pairs.astype(jnp.float32)
    real = scratch[pl.ds(0, count, stride=2), :]
    imag = scratch[pl.ds(1, count, stride=2), :]
    return jnp.concatenate([real, imag], axis=1).astype(jnp.bfloat16)


def share_kernel(picks, share, out, scratch):
    for y in range(YS):
        piece = split_pairs(share[0, 256 * y : 256 * y + 256, :], scratch)
        out[0, y % 2, 128 * (y // 2) : 128 * (y // 2) + 128, :] = piece


def split_share(picks, share):
    return pl.pallas_call(
        share_kernel,
        out_shape=jax.ShapeDtypeStruct((XS, 2, 512, 256), jnp.bfloat16),
        grid_spec=pltpu.PrefetchScalarGridSpec(
            num_scalar_prefetch=1,
            grid=(XS,),
            in_specs=[pl.BlockSpec((1, 2048, 128), lambda k, picks: (picks[0], k, 0))],
            out_specs=pl.BlockSpec((1, 2, 512, 256), lambda k, picks: (k, 0, 0, 0)),
            scratch_shapes=[pltpu.VMEM((256, 128), jnp.float32)],
        ),
        name="split_share",
        cost_estimate=pl.CostEstimate(flops=400_000_000, bytes_accessed=4_200_000, transcendentals=0),
        interpret=INTERPRET,
    )(picks, share)


def wide(chunk):
    return jnp.concatenate([chunk[q, :ROWS, :] for q in range(QUADS)], axis=1)


def dot(a, b):
    return jnp.dot(a, b, preferred_element_type=jnp.float32)


EARLY = ((0, True), (0, False), (-1, True), (1, True), (1, False), (2, False))
LATE = ((2, True), (-1, False))


def block_of(picks, kind):
    offset, same = kind
    x = (picks[1] + offset + XS) % XS
    return x, picks[2] if same else 1 - picks[2]


def early_kernel(picks, share, c0, c1, c2, c3, c4, c5, acc):
    for n, (chunk, kind) in enumerate(zip((c0, c1, c2, c3, c4, c5), EARLY)):
        x, parity = block_of(picks, kind)
        term = dot(wide(chunk), share[x, parity])
        if n == 0:
            acc[...] = term
        else:
            acc[...] += term


def early_product(picks, share, chunks):
    return pl.pallas_call(
        early_kernel,
        out_shape=jax.ShapeDtypeStruct((ROWS, 256), jnp.float32),
        in_specs=[pl.BlockSpec(memory_space=pltpu.SMEM)] + [pl.BlockSpec(memory_space=pltpu.VMEM)] * 7,
        out_specs=pl.BlockSpec(memory_space=pltpu.VMEM),
        name="early_product",
        cost_estimate=pl.CostEstimate(flops=400_000_000, bytes_accessed=4_200_000, transcendentals=0),
        interpret=INTERPRET,
    )(picks, share, *chunks)


def late_kernel(
    picks, weights, share, spread, before, c0, c1, c2, c3, c4, c5, c6, c7, kept, sent,
    acc, blocks, small, ends, late, extra, acc_extra, scratch, sems,
):
    early = (c0, c1, c2, c3, c4, c5)
    chunks = (c6, c7)
    copies = []

    def start(source, target):
        copy = pltpu.make_async_copy(source, target, sems.at[len(copies)])
        copy.start()
        copies.append(copy)

    for e in range(EXTRAS):
        start(spread.at[picks[4 + e]], small.at[e])
    for n in range(6):
        start(early[n].at[:, pl.ds(ROWS, 80), :], ends.at[n])
    for n in range(2):
        x, parity = block_of(picks, LATE[n])
        start(chunks[n], late.at[n])
        start(share.at[x, parity], blocks.at[n])
    start(before, acc)

    def place(rows_of, kind):
        x, parity = block_of(picks, kind)
        for q in range(QUADS):
            rows = rows_of(q)
            at = pl.multiple_of(8 * (YS * x + 2 * q + parity), 8)
            for v in range(9):
                extra[pl.ds(at, 8), 128 * v : 128 * v + 128] = rows[8 * v : 8 * v + 8]

    for copy in copies[:9]:
        copy.wait()
    for n in range(6):
        place(lambda q: ends[n, q].astype(jnp.float32), EARLY[n])
    slices = [split_pairs(small[e], scratch) for e in range(EXTRAS)]
    for n in range(2):
        copies[9 + 2 * n].wait()
        place(lambda q: late[n, q, ROWS:, :].astype(jnp.float32), LATE[n])
    for e in range(EXTRAS):
        turned = extra[:, ROWS * e : ROWS * e + ROWS].astype(jnp.bfloat16)
        acc_extra[e] = lax.dot_general(
            turned, slices[e], (((0,), (0,)), ((), ())), preferred_element_type=jnp.float32
        )
    copies[13].wait()
    for n in range(2):
        copies[10 + 2 * n].wait()
        acc[...] += dot(wide(late.at[n]), blocks[n])

    upper = lax.broadcasted_iota(jnp.int32, (8, 128), 0) < 4

    def decode(g):
        top = [jnp.zeros((8, 128), jnp.float32)] * 4
        low = [jnp.zeros((8, 128), jnp.float32)] * 4
        at = pl.multiple_of(24 * g, 8)
        for s in range(1 + EXTRAS):
            tiles = [
                acc[pl.ds(at + 8 * v, 8), :] if s == 0 else acc_extra[s - 1, pl.ds(at + 8 * v, 8), :]
                for v in range(3)
            ]
            top_r = tiles[0][:, :128] - tiles[1][:, 128:]
            top_i = tiles[0][:, 128:] + tiles[1][:, :128]
            low_r = tiles[2][:, :128] - pltpu.roll(tiles[2][:, 128:], 4, 0)
            low_i = tiles[2][:, 128:] + pltpu.roll(tiles[2][:, :128], 4, 0)
            for b in range(4):
                w_r = weights[8 * s + b : 8 * s + b + 1, :]
                w_i = weights[8 * s + 4 + b : 8 * s + 5 + b, :]
                top[b] = top[b] + (w_r * top_r - w_i * top_i)
                low[b] = low[b] + (w_r * low_r - w_i * low_i)
        low_a = jnp.where(upper, low[0], pltpu.roll(low[1], 4, 0))
        low_b = jnp.where(upper, low[2], pltpu.roll(low[3], 4, 0))
        return jnp.concatenate(top + [low_a, low_b], axis=0)

    core = picks[3]

    def both(z, carry):
        kept[z] = decode(2 * z + core)
        sent[z] = decode(2 * z + 1 - core)
        return carry

    lax.fori_loop(0, PAIRS // 2, both, 0)


def late_product(picks, weights, share, spread, before, early, late):
    return pl.pallas_call(
        late_kernel,
        out_shape=(jax.ShapeDtypeStruct((PAIRS // 2, 48, 128), jnp.float32),) * 2,
        in_specs=[pl.BlockSpec(memory_space=pltpu.SMEM), pl.BlockSpec(memory_space=pltpu.VMEM)]
        + [pl.BlockSpec(memory_space=pl.ANY)] * 11,
        out_specs=(pl.BlockSpec(memory_space=pltpu.VMEM),) * 2,
        scratch_shapes=[
            pltpu.VMEM((ROWS, 256), jnp.float32),
            pltpu.VMEM((2, 512, 256), jnp.bfloat16),
            pltpu.VMEM((EXTRAS, 512, 128), jnp.bfloat16),
            pltpu.VMEM((6, QUADS, 80, 128), jnp.bfloat16),
            pltpu.VMEM((2, QUADS, CHUNK_ROWS, 128), jnp.bfloat16),
            pltpu.VMEM((256, 1152), jnp.float32),
            pltpu.VMEM((EXTRAS, ROWS, 256), jnp.float32),
            pltpu.VMEM((512, 128), jnp.float32),
            pltpu.SemaphoreType.DMA((14,)),
        ],
        name="late_product",
        interpret=INTERPRET,
    )(picks, weights, share, spread, before, *early, *late)


def summed(received):
    total = jnp.sum(received, axis=0)
    top = total[:32].reshape(2, 2, 8, 128)
    low = total[32:].reshape(2, 2, 4, 128)
    return jnp.concatenate([top, low], axis=2).transpose(0, 2, 1, 3)


def shards(source_matrix_tiles, second_operand_encoded, responding_nodes):
    group = ("z", "core")
    sent, picks = encode(
        responding_nodes,
        jnp.asarray(trig_table().reshape(-1)),
        source_matrix_tiles.reshape(96, 128),
    )
    got = lax.all_to_all(sent, group, split_axis=0, concat_axis=0, tiled=True)

    odd = second_operand_encoded[1].reshape(PANELS, PAIRS, 8, 2, 128).transpose(1, 0, 2, 3, 4)
    odd, got = lax.optimization_barrier((odd, got))
    spread = lax.all_to_all(odd, group, split_axis=0, concat_axis=0, tiled=True)
    a = lax.all_gather(compact(got), "quad")

    def hop(chunk, axis, size, by):
        return lax.ppermute(chunk, axis, [(i, (i + by) % size) for i in range(size)])

    y_axes = ("quad", "parity")
    nodes, whole, a = lax.optimization_barrier((responding_nodes, second_operand_encoded, a))
    right_a = hop(a, "x", XS, 1)
    left_a = hop(a, "x", XS, -1)
    b = hop(a, y_axes, YS, 1)
    right_b = hop(right_a, y_axes, YS, -1)
    left_b = hop(left_a, y_axes, YS, -1)
    far_a = hop(right_a, "x", XS, 1)
    slant = [(YS * x + y, YS * ((x - 1) % XS) + (y + 1) % YS) for x in range(XS) for y in range(YS)]
    far_b = lax.ppermute(left_a, ("x",) + y_axes, slant)
    share = split_share(picks, whole.reshape(2, 8192, 128))
    weights = decode_weights(nodes, picks)
    early = (a, b, right_a, left_a, left_b, far_b)
    before = early_product(picks, share, early)
    kept, passed = late_product(
        picks, weights, share, spread.reshape(PAIRS, 512, 128), before, early, (far_a, right_b)
    )
    kept = kept + lax.ppermute(passed, "core", [(0, 1), (1, 0)])
    received = lax.all_to_all(kept, "z", split_axis=0, concat_axis=0, tiled=True)
    return summed(received)


def solution(mesh):
    torus = Mesh(
        mesh.devices.reshape(PAIRS // 2, 2, XS, QUADS, 2), ("z", "core", "x", "quad", "parity")
    )
    group = ("z", "core")
    panel = ("x", "quad", "parity")
    return jax.shard_map(
        shards,
        mesh=torus,
        in_specs=(P(None, group, None, panel), P(group, None, None, panel), P()),
        out_specs=P(None, group, None, panel),
        check_vma=False,
    )
```

```python
import math

import jax
import jax.numpy as jnp
import numpy as np
from jax import lax
from jax.experimental import pallas as pl
from jax.experimental.pallas import tpu as pltpu
from jax.sharding import Mesh
from jax.sharding import PartitionSpec as P


NODE_NUMBER = 32
PAIRS = 16
EXTRAS = 3
XS = 4
YS = 8
QUADS = YS // 2
PANELS = XS * YS
ROWS = 384
CHUNK_ROWS = 464
INTERPRET = False

TWO_PI_RADIANS = 2.0 * math.pi


def trig_table():
    exponent = np.arange(4, dtype=np.float32)[None, :] + 8 * np.arange(2, dtype=np.float32)[:, None]
    point = np.arange(NODE_NUMBER, dtype=np.float32)
    phase = np.float32(TWO_PI_RADIANS) * point / np.float32(NODE_NUMBER)
    angle = (phase[:, None, None] * exponent[None]).astype(np.float64)
    table = np.stack([np.cos(angle), np.sin(angle)], axis=1)
    return table.reshape(NODE_NUMBER, 16).astype(np.float32)


def grid_table():
    grid = np.float32(TWO_PI_RADIANS) * np.arange(NODE_NUMBER, dtype=np.float32) / np.float32(NODE_NUMBER)
    wanted = (3 + 4 * np.arange(4)).astype(np.float32)
    turns = (-grid[None, :] * wanted[:, None]).astype(np.float64)
    grid = grid.astype(np.float64)
    rows = np.zeros((16, 128), np.float32)
    rows[0, :NODE_NUMBER] = np.cos(grid)
    rows[1, :NODE_NUMBER] = np.sin(grid)
    rows[2:6, :NODE_NUMBER] = np.cos(turns)
    rows[6:10, :NODE_NUMBER] = np.sin(turns)
    return rows


def weights_kernel(nodes, picks, points, grid, out):
    number = nodes.shape[0]
    shape = (24, 128)
    row = lax.broadcasted_iota(jnp.int32, shape, 0)
    lane = lax.broadcasted_iota(jnp.int32, shape, 1)
    real = jnp.ones(shape, jnp.float32)
    imag = jnp.zeros(shape, jnp.float32)
    node = jnp.full(shape, -1, jnp.int32)
    for t in range(number):
        mine = row == t
        node = jnp.where(mine, nodes[t], node)
        step_r = jnp.where(mine, 1.0, grid[0:1, :] - points[nodes[t]])
        step_i = jnp.where(mine, 0.0, grid[1:2, :] - points[NODE_NUMBER + nodes[t]])
        real, imag = real * step_r - imag * step_i, real * step_i + imag * step_r

    def across(value):
        return jnp.sum(value, axis=1, keepdims=True)

    here = node == lane
    denom_r = across(jnp.where(here, real, 0.0))
    denom_i = across(jnp.where(here, imag, 0.0))
    magnitude = denom_r * denom_r + denom_i * denom_i
    for e in range(4):
        cos, sin = grid[2 + e : 3 + e, :], grid[6 + e : 7 + e, :]
        numer_r = across(real * cos - imag * sin) / NODE_NUMBER
        numer_i = across(real * sin + imag * cos) / NODE_NUMBER
        weight_r = (numer_r * denom_r + numer_i * denom_i) / magnitude
        weight_i = (numer_i * denom_r - numer_r * denom_i) / magnitude
        for c in range(1 + EXTRAS):
            chosen = node == picks[8 + c]
            out[8 * c + e : 8 * c + e + 1, :] = jnp.sum(
                jnp.where(chosen, weight_r, 0.0), axis=0, keepdims=True
            )
            out[8 * c + 4 + e : 8 * c + 5 + e, :] = jnp.sum(
                jnp.where(chosen, weight_i, 0.0), axis=0, keepdims=True
            )


def decode_weights(nodes, picks):
    grid = grid_table()
    points = grid[:2, :NODE_NUMBER].reshape(-1)
    return pl.pallas_call(
        weights_kernel,
        out_shape=jax.ShapeDtypeStruct((32, 128), jnp.float32),
        in_specs=[pl.BlockSpec(memory_space=pltpu.SMEM)] * 3 + [pl.BlockSpec(memory_space=pltpu.VMEM)],
        out_specs=pl.BlockSpec(memory_space=pltpu.VMEM),
        name="weights",
        interpret=INTERPRET,
    )(nodes, picks, jnp.asarray(points), jnp.asarray(grid))


def position():
    group = 2 * lax.axis_index("z") + lax.axis_index("core")
    return group, lax.axis_index("x"), lax.axis_index("parity")


def encode_kernel(nodes, table, source, out, picks, flags, extra_points, rows, stack):
    for j in range(NODE_NUMBER):
        flags[j] = 0
    for s in range(nodes.shape[0]):
        flags[nodes[s]] = 1
    found = jnp.int32(0)
    for g in range(PAIRS):
        extra_points[found] = 2 * g + 1
        found = found + flags[2 * g] * flags[2 * g + 1]
    group, x, parity = position()
    second = 1 - flags[2 * group]
    picks[0] = second
    picks[1] = x
    picks[2] = parity
    picks[3] = group % 2
    picks[8] = 2 * group + second
    for e in range(EXTRAS):
        picks[4 + e] = (extra_points[e] - 1) // 2
        picks[9 + e] = extra_points[e]

    rows[...] = source[...].astype(jnp.float32)
    tops = []
    lows = []
    for b in range(8):
        at = 48 * (b // 4) + b % 4
        tops.append(rows[pl.ds(at, 8, stride=4), :])
        low = rows[pl.ds(at + 32, 4, stride=4), :]
        lows.append(jnp.concatenate([low, low], axis=0))
    upper = lax.broadcasted_iota(jnp.int32, (8, 128), 0) < 4

    def block(point):
        at = 16 * point
        real = [table[at + b] for b in range(8)]
        imag = [table[at + 8 + b] for b in range(8)]
        top_r = sum(real[b] * tops[b] for b in range(8))
        top_i = sum(imag[b] * tops[b] for b in range(8))
        low = sum(jnp.where(upper, real[b], imag[b]) * lows[b] for b in range(8))
        return [top_r, top_i, low]

    stack[...] = jnp.zeros_like(stack)
    for e in range(EXTRAS):
        for v, tile in enumerate(block(extra_points[e])):
            stack[24 * e + 8 * v : 24 * e + 8 * v + 8, :] = tile
    stack[...] = stack[...].T

    def main(t, carry):
        parts = block(2 * t + 1 - flags[2 * t])
        parts.append(stack[pl.ds(pl.multiple_of(8 * t, 8), 8), :])
        value = jnp.concatenate(parts, axis=0).astype(jnp.bfloat16)
        out[t] = value
        return carry

    lax.fori_loop(0, PAIRS, main, 0)


def encode(nodes, table, source):
    return pl.pallas_call(
        encode_kernel,
        out_shape=(
            jax.ShapeDtypeStruct((PAIRS, 32, 128), jnp.bfloat16),
            jax.ShapeDtypeStruct((16,), jnp.int32),
        ),
        in_specs=[pl.BlockSpec(memory_space=pltpu.SMEM)] * 2 + [pl.BlockSpec(memory_space=pltpu.VMEM)],
        out_specs=(pl.BlockSpec(memory_space=pltpu.VMEM), pl.BlockSpec(memory_space=pltpu.SMEM)),
        scratch_shapes=[
            pltpu.SMEM((NODE_NUMBER,), jnp.int32),
            pltpu.SMEM((PAIRS,), jnp.int32),
            pltpu.VMEM((96, 128), jnp.float32),
            pltpu.VMEM((128, 128), jnp.float32),
        ],
        name="encode",
        interpret=INTERPRET,
    )(nodes, table, source)


def compact_kernel(got, out, rows):
    lane = lax.broadcasted_iota(jnp.int32, (8, 128), 1)
    rows[ROWS + 72 :, :] = jnp.zeros((8, 128), jnp.float32)
    pieces = []
    for g in range(PAIRS):
        block = got[g].astype(jnp.float32)
        rows[24 * g : 24 * g + 24, :] = block[:24]
        pieces.append(block[24:])
    for e in range(EXTRAS):
        for v in range(3):
            tile = jnp.zeros((8, 128), jnp.float32)
            for g in range(PAIRS):
                start = 24 * g - 128 * v
                if start + 24 <= 0 or start >= 128:
                    continue
                moved = pltpu.roll(pieces[g], (start - 24 * e) % 128, 1)
                tile = jnp.where((lane >= start) & (lane < start + 24), moved, tile)
            at = ROWS + 8 * (3 * e + v)
            rows[at : at + 8, :] = tile
    out[...] = rows[...].astype(jnp.bfloat16)


def compact(got):
    return pl.pallas_call(
        compact_kernel,
        out_shape=jax.ShapeDtypeStruct((CHUNK_ROWS, 128), jnp.bfloat16),
        in_specs=[pl.BlockSpec(memory_space=pltpu.VMEM)],
        out_specs=pl.BlockSpec(memory_space=pltpu.VMEM),
        scratch_shapes=[pltpu.VMEM((CHUNK_ROWS, 128), jnp.float32)],
        name="compact",
        interpret=INTERPRET,
    )(got)


def split_pairs(pairs, scratch):
    count = pairs.shape[0] // 2
    scratch[: 2 * count, :] = pairs.astype(jnp.float32)
    real = scratch[pl.ds(0, count, stride=2), :]
    imag = scratch[pl.ds(1, count, stride=2), :]
    return jnp.concatenate([real, imag], axis=1).astype(jnp.bfloat16)


def share_kernel(picks, share, out, scratch):
    for y in range(YS):
        piece = split_pairs(share[0, 256 * y : 256 * y + 256, :], scratch)
        out[0, y % 2, 128 * (y // 2) : 128 * (y // 2) + 128, :] = piece


def split_share(picks, share):
    return pl.pallas_call(
        share_kernel,
        out_shape=jax.ShapeDtypeStruct((XS, 2, 512, 256), jnp.bfloat16),
        grid_spec=pltpu.PrefetchScalarGridSpec(
            num_scalar_prefetch=1,
            grid=(XS,),
            in_specs=[pl.BlockSpec((1, 2048, 128), lambda k, picks: (picks[0], k, 0))],
            out_specs=pl.BlockSpec((1, 2, 512, 256), lambda k, picks: (k, 0, 0, 0)),
            scratch_shapes=[pltpu.VMEM((256, 128), jnp.float32)],
        ),
        name="split_share",
        cost_estimate=pl.CostEstimate(flops=400_000_000, bytes_accessed=4_200_000, transcendentals=0),
        interpret=INTERPRET,
    )(picks, share)


def wide(chunk):
    return jnp.concatenate([chunk[q, :ROWS, :] for q in range(QUADS)], axis=1)


def dot(a, b):
    return jnp.dot(a, b, preferred_element_type=jnp.float32)


EARLY = ((0, True), (0, False), (-1, True), (1, True), (1, False), (2, False))
LATE = ((2, True), (-1, False))


def block_of(picks, kind):
    offset, same = kind
    x = (picks[1] + offset + XS) % XS
    return x, picks[2] if same else 1 - picks[2]


def early_kernel(picks, share, c0, c1, c2, c3, c4, c5, spread, acc):
    for n, (chunk, kind) in enumerate(zip((c0, c1, c2, c3, c4, c5), EARLY)):
        x, parity = block_of(picks, kind)
        term = dot(wide(chunk), share[x, parity])
        if n == 0:
            acc[...] = term
        else:
            acc[...] += term


def early_product(picks, share, chunks, spread):
    return pl.pallas_call(
        early_kernel,
        out_shape=jax.ShapeDtypeStruct((ROWS, 256), jnp.float32),
        in_specs=[pl.BlockSpec(memory_space=pltpu.SMEM)] + [pl.BlockSpec(memory_space=pltpu.VMEM)] * 7
        + [pl.BlockSpec(memory_space=pl.ANY)],
        out_specs=pl.BlockSpec(memory_space=pltpu.VMEM),
        name="early_product",
        cost_estimate=pl.CostEstimate(flops=400_000_000, bytes_accessed=4_200_000, transcendentals=0),
        interpret=INTERPRET,
    )(picks, share, *chunks, spread)


def late_kernel(
    picks, weights, share, spread, before, c0, c1, c2, c3, c4, c5, c6, c7, kept, sent,
    acc, blocks, small, ends, late, extra, acc_extra, scratch, sems,
):
    early = (c0, c1, c2, c3, c4, c5)
    chunks = (c6, c7)
    copies = []

    def start(source, target):
        copy = pltpu.make_async_copy(source, target, sems.at[len(copies)])
        copy.start()
        copies.append(copy)

    for e in range(EXTRAS):
        start(spread.at[picks[4 + e]], small.at[e])
    for n in range(6):
        start(early[n].at[:, pl.ds(ROWS, 80), :], ends.at[n])
    for n in range(2):
        x, parity = block_of(picks, LATE[n])
        start(chunks[n], late.at[n])
        start(share.at[x, parity], blocks.at[n])
    start(before, acc)

    def place(rows_of, kind):
        x, parity = block_of(picks, kind)
        for q in range(QUADS):
            rows = rows_of(q)
            at = pl.multiple_of(8 * (YS * x + 2 * q + parity), 8)
            for v in range(9):
                extra[pl.ds(at, 8), 128 * v : 128 * v + 128] = rows[8 * v : 8 * v + 8]

    for copy in copies[:9]:
        copy.wait()
    for n in range(6):
        place(lambda q: ends[n, q].astype(jnp.float32), EARLY[n])
    slices = [split_pairs(small[e], scratch) for e in range(EXTRAS)]
    for n in range(2):
        copies[9 + 2 * n].wait()
        place(lambda q: late[n, q, ROWS:, :].astype(jnp.float32), LATE[n])
    for e in range(EXTRAS):
        turned = extra[:, ROWS * e : ROWS * e + ROWS].astype(jnp.bfloat16)
        acc_extra[e] = lax.dot_general(
            turned, slices[e], (((0,), (0,)), ((), ())), preferred_element_type=jnp.float32
        )
    copies[13].wait()
    for n in range(2):
        copies[10 + 2 * n].wait()
        acc[...] += dot(wide(late.at[n]), blocks[n])

    upper = lax.broadcasted_iota(jnp.int32, (8, 128), 0) < 4

    def decode(g):
        top = [jnp.zeros((8, 128), jnp.float32)] * 4
        low = [jnp.zeros((8, 128), jnp.float32)] * 4
        at = pl.multiple_of(24 * g, 8)
        for s in range(1 + EXTRAS):
            tiles = [
                acc[pl.ds(at + 8 * v, 8), :] if s == 0 else acc_extra[s - 1, pl.ds(at + 8 * v, 8), :]
                for v in range(3)
            ]
            top_r = tiles[0][:, :128] - tiles[1][:, 128:]
            top_i = tiles[0][:, 128:] + tiles[1][:, :128]
            low_r = tiles[2][:, :128] - pltpu.roll(tiles[2][:, 128:], 4, 0)
            low_i = tiles[2][:, 128:] + pltpu.roll(tiles[2][:, :128], 4, 0)
            for b in range(4):
                w_r = weights[8 * s + b : 8 * s + b + 1, :]
                w_i = weights[8 * s + 4 + b : 8 * s + 5 + b, :]
                top[b] = top[b] + (w_r * top_r - w_i * top_i)
                low[b] = low[b] + (w_r * low_r - w_i * low_i)
        low_a = jnp.where(upper, low[0], pltpu.roll(low[1], 4, 0))
        low_b = jnp.where(upper, low[2], pltpu.roll(low[3], 4, 0))
        return jnp.concatenate(top + [low_a, low_b], axis=0)

    core = picks[3]

    def both(z, carry):
        kept[z] = decode(2 * z + core)
        sent[z] = decode(2 * z + 1 - core)
        return carry

    lax.fori_loop(0, PAIRS // 2, both, 0)


def late_product(picks, weights, share, spread, before, early, late):
    return pl.pallas_call(
        late_kernel,
        out_shape=(jax.ShapeDtypeStruct((PAIRS // 2, 48, 128), jnp.float32),) * 2,
        in_specs=[pl.BlockSpec(memory_space=pltpu.SMEM), pl.BlockSpec(memory_space=pltpu.VMEM)]
        + [pl.BlockSpec(memory_space=pl.ANY)] * 11,
        out_specs=(pl.BlockSpec(memory_space=pltpu.VMEM),) * 2,
        scratch_shapes=[
            pltpu.VMEM((ROWS, 256), jnp.float32),
            pltpu.VMEM((2, 512, 256), jnp.bfloat16),
            pltpu.VMEM((EXTRAS, 512, 128), jnp.bfloat16),
            pltpu.VMEM((6, QUADS, 80, 128), jnp.bfloat16),
            pltpu.VMEM((2, QUADS, CHUNK_ROWS, 128), jnp.bfloat16),
            pltpu.VMEM((256, 1152), jnp.float32),
            pltpu.VMEM((EXTRAS, ROWS, 256), jnp.float32),
            pltpu.VMEM((512, 128), jnp.float32),
            pltpu.SemaphoreType.DMA((14,)),
        ],
        name="late_product",
        interpret=INTERPRET,
    )(picks, weights, share, spread, before, *early, *late)


def summed(received):
    total = jnp.sum(received, axis=0)
    top = total[:32].reshape(2, 2, 8, 128)
    low = total[32:].reshape(2, 2, 4, 128)
    return jnp.concatenate([top, low], axis=2).transpose(0, 2, 1, 3)


def shards(source_matrix_tiles, second_operand_encoded, responding_nodes):
    group = ("z", "core")
    sent, picks = encode(
        responding_nodes,
        jnp.asarray(trig_table().reshape(-1)),
        source_matrix_tiles.reshape(96, 128),
    )
    got = lax.all_to_all(sent, group, split_axis=0, concat_axis=0, tiled=True)

    odd = second_operand_encoded[1].reshape(PANELS, PAIRS, 8, 2, 128).transpose(1, 0, 2, 3, 4)
    odd, got = lax.optimization_barrier((odd, got))
    spread = lax.all_to_all(odd, group, split_axis=0, concat_axis=0, tiled=True)
    a = lax.all_gather(compact(got), "quad")

    def hop(chunk, axis, size, by):
        return lax.ppermute(chunk, axis, [(i, (i + by) % size) for i in range(size)])

    y_axes = ("quad", "parity")
    nodes, whole, a = lax.optimization_barrier((responding_nodes, second_operand_encoded, a))
    right_a = hop(a, "x", XS, 1)
    left_a = hop(a, "x", XS, -1)
    b = hop(a, y_axes, YS, -1)
    right_b = hop(right_a, y_axes, YS, 1)
    left_b = hop(left_a, y_axes, YS, -1)
    far_a = hop(right_a, "x", XS, 1)
    slant = [(YS * x + y, YS * ((x - 1) % XS) + (y + 1) % YS) for x in range(XS) for y in range(YS)]
    far_b = lax.ppermute(left_a, ("x",) + y_axes, slant)
    share = split_share(picks, whole.reshape(2, 8192, 128))
    weights = decode_weights(nodes, picks)
    early = (a, b, right_a, left_a, left_b, far_b)
    spread = spread.reshape(PAIRS, 512, 128)
    before = early_product(picks, share, early, spread)
    kept, passed = late_product(
        picks, weights, share, spread, before, early, (far_a, right_b)
    )
    kept = kept + lax.ppermute(passed, "core", [(0, 1), (1, 0)])
    received = lax.all_to_all(kept, "z", split_axis=0, concat_axis=0, tiled=True)
    return summed(received)


def solution(mesh):
    torus = Mesh(
        mesh.devices.reshape(PAIRS // 2, 2, XS, QUADS, 2), ("z", "core", "x", "quad", "parity")
    )
    group = ("z", "core")
    panel = ("x", "quad", "parity")
    return jax.shard_map(
        shards,
        mesh=torus,
        in_specs=(P(None, group, None, panel), P(group, None, None, panel), P()),
        out_specs=P(None, group, None, panel),
        check_vma=False,
    )
```
